128 devices in a mesh: mem: 4 (over y_lo, core), lat: 4 (over z), lon: 8 (over y_hi, x).
Axes of the slice: x: 4, y: 4 (y_hi: 2, y_lo: 2; y = y_hi * 2 + y_lo), z: 4, core: 2. Of those that a mesh axis runs over, the one named last changes fastest.
Arguments:
- fields: bfloat16 [4, 2, 96, 384, 512], P('mem', None, 'lat', 'lon'), may hold values from -6 to 6
- region: int32 [96, 384], P('lat', 'lon'), may hold values from 0 to 2
- gain_attn: float32 [512], replicated, may hold values from 0.1 to 1.9
- w_qkv: bfloat16 [512, 1536], P(None, ('mem', 'lat', 'lon')), may hold values from -1 to 1
- w_proj: bfloat16 [512, 512], P(None, ('mem', 'lat', 'lon')), may hold values from -0.25 to 0.25
- gain_mlp: float32 [512], replicated, may hold values from 0.1 to 1.9
- w_up: bfloat16 [512, 2048], P(None, ('mem', 'lat', 'lon')), may hold values from -0.25 to 0.25
- w_down: bfloat16 [2048, 512], P(None, ('mem', 'lat', 'lon')), may hold values from -0.125 to 0.125
Outputs:
- updated: bfloat16 [4, 2, 96, 384, 512], P('mem', None, 'lat', 'lon')
The draws below stay inside these ranges and needn't reach their ends.
All inputs are finite; a program needn't handle non-finite values.
Results may differ from the reference program's by a relative error of at most 0.011.
Values may be sent and summed in bfloat16 or wider, within the bound.
No kernel may reach another device: no remote copies, remote signals or barrier semaphores. Data moves between devices by JAX's collectives and lax.ppermute only.
A program may use at most 192 MiB of HBM per device.

```python
import jax
import jax.numpy as jnp
from jax import lax

D = 512
HEADS = 16
FF = 2048
HDIM = 32
WLAT = 6
WLON = 12
LEVELS = 2
SH = 3
SL = 6
MEMBERS = 4
NLAT = 96
NLON = 384


def draw_w_qkv(key, part):
    first = jax.random.fold_in(key, 11)
    drawn = jnp.clip(jax.random.normal(first, (D, 3 * D), jnp.float32), -6.0, 6.0) / D ** 0.5
    return drawn.astype(jnp.bfloat16)


def with_ends(array, key, least, top_value):
    shape = array.shape
    index_at = [jax.random.randint(jax.random.fold_in(key, axis), (), 0, shape[axis]) for axis in range(len(shape))]
    array = array.at[tuple(index_at)].set(least)
    longest = shape.index(max(shape))
    index_at[longest] = (index_at[longest] + 1) % shape[longest]
    return array.at[tuple(index_at)].set(top_value)


def levels(own_key, dims, split, low, largest):
    factor_of = 1.0
    for axis_at, blocks in split:
        heights = jax.random.uniform(jax.random.fold_in(jax.random.fold_in(own_key, 6), axis_at), (blocks,), jnp.float32, low / len(split), largest / len(split))
        factor_of = factor_of * jnp.repeat(jnp.exp(heights), dims[axis_at] // blocks).reshape((-1,) + (1,) * (len(dims) - 1 - axis_at))
    return factor_of


def scatter_about(rng, dims, deviation, most, split=(), held_as=jnp.bfloat16):
    drawn = deviation * jax.random.normal(rng, dims, jnp.float32)
    if split:
        drawn = drawn * levels(rng, dims, split, -0.22, 0.18)
    return jnp.clip(drawn, -most, most).astype(held_as)


def setup_inputs(seed: int = 0) -> dict:
    splits = jax.random.split(jax.random.key(seed), 9)
    fields = scatter_about(splits[0], (MEMBERS, LEVELS, NLAT, NLON, D), 1.0, 6.0, ((0, 4), (2, 4), (3, 8)))
    region = with_ends(jax.random.randint(splits[1], (NLAT, NLON), 0, 3), jax.random.fold_in(splits[1], 1), 0, 2).astype(jnp.int32)
    gain_attn = jnp.clip(1.0 + 0.18 * jax.random.normal(splits[2], (D,), jnp.float32), 0.1, 1.9)
    w_qkv = draw_w_qkv(jax.random.fold_in(splits[8], 71), 0)
    w_proj = scatter_about(splits[4], (D, D), D ** -0.5, 0.25, ((1, 128),))
    gain_mlp = jnp.clip(1.0 + 0.18 * jax.random.normal(splits[5], (D,), jnp.float32), 0.1, 1.9)
    w_up = scatter_about(splits[6], (D, FF), D ** -0.5, 0.25, ((1, 128),))
    w_down = scatter_about(splits[7], (FF, D), FF ** -0.5, 0.125, ((1, 128),))
    return dict(fields=fields, region=region, gain_attn=gain_attn, w_qkv=w_qkv, w_proj=w_proj, gain_mlp=gain_mlp, w_up=w_up, w_down=w_down)


eps = 1e-05

def layer_norm(values, gain_vec):
    values = values.astype(jnp.float32)
    average = lax.optimization_barrier(jnp.mean(values, axis=-1, keepdims=True))
    centred = values - average
    variance = lax.optimization_barrier(jnp.mean(centred * centred, axis=-1, keepdims=True))
    return (centred * lax.rsqrt(variance + eps) * gain_vec).astype(jnp.bfloat16)

def to_windows(arr):
    chans = arr.shape[-1]
    arr = arr.reshape(LEVELS, NLAT // WLAT, WLAT, NLON // WLON, WLON, chans)
    arr = arr.transpose(1, 3, 0, 2, 4, 5)
    return arr.reshape(NLAT // WLAT, NLON // WLON, LEVELS * WLAT * WLON, chans)

def reference(fields, region, gain_attn, w_qkv, w_proj, gain_mlp, w_up, w_down):
    scale = 1.0 / HDIM ** 0.5
    win_tok = LEVELS * WLAT * WLON
    shifted_ids = jnp.roll(region, (-SH, -SL), axis=(0, 1)).astype(jnp.int32)
    north = ((jnp.arange(NLAT) + SH) % NLAT < SH).astype(jnp.int32)
    ids_win = to_windows(jnp.broadcast_to(shifted_ids[None, :, :, None], (LEVELS, NLAT, NLON, 1)))[..., 0]
    north_win = to_windows(jnp.broadcast_to(north[None, :, None, None], (LEVELS, NLAT, NLON, 1)))[..., 0]

    def band_fn(args):
        tokens, ids_band, north_band = args
        count = tokens.shape[0]
        qkv_all = jnp.dot(tokens.reshape(-1, D), w_qkv, preferred_element_type=jnp.float32).astype(jnp.bfloat16)
        qkv_all = qkv_all.reshape(count, win_tok, 3, HEADS, HDIM).astype(jnp.float32)
        queries = qkv_all[:, :, 0]
        keys_in = qkv_all[:, :, 1]
        values_in = qkv_all[:, :, 2]
        scores = jnp.einsum('wqhd,wkhd->whqk', queries, keys_in) * scale
        allow = (ids_band[:, :, None] == ids_band[:, None, :]) & (north_band[:, :, None] == north_band[:, None, :])
        scores = jnp.where(allow[:, None], scores, -1000000000.0)
        attn_probs = jax.nn.softmax(scores, axis=-1).astype(jnp.bfloat16)
        mixed_heads = jnp.einsum('whqk,wkhd->wqhd', attn_probs.astype(jnp.float32), values_in).astype(jnp.bfloat16)
        mixed_heads = mixed_heads.reshape(count * win_tok, D)
        projected = jnp.dot(mixed_heads, w_proj, preferred_element_type=jnp.float32).astype(jnp.bfloat16)
        return projected.reshape(count, win_tok, D)

    def one_member(member):
        normed = layer_norm(member, gain_attn)
        shifted = jnp.roll(normed, (-SH, -SL), axis=(1, 2))
        out_win = lax.map(band_fn, (to_windows(shifted), ids_win, north_win))
        out_win = out_win.reshape(NLAT // WLAT, NLON // WLON, LEVELS, WLAT, WLON, D)
        attn_out = out_win.transpose(2, 0, 3, 1, 4, 5).reshape(LEVELS, NLAT, NLON, D)
        attn_out = jnp.roll(attn_out, (SH, SL), axis=(1, 2))
        resid = (member.astype(jnp.float32) + attn_out.astype(jnp.float32)).astype(jnp.bfloat16)
        normed2 = layer_norm(resid, gain_mlp).reshape(-1, D)
        hidden = jax.nn.gelu(jnp.dot(normed2, w_up, preferred_element_type=jnp.float32), approximate=False).astype(jnp.bfloat16)
        delta = jnp.dot(hidden, w_down, preferred_element_type=jnp.float32).reshape(LEVELS, NLAT, NLON, D)
        return (resid.astype(jnp.float32) + delta).astype(jnp.bfloat16)
    return lax.map(one_member, fields)
```

```python
import functools
import math

import jax
import jax.numpy as jnp
import numpy as np
from jax import lax
from jax.experimental import pallas as pl
from jax.experimental.pallas import tpu as pltpu
from jax.sharding import PartitionSpec as P

D = 512
HDIM = 32
FF = 2048
SH = 3
SL = 6
TOK = 144
EDGE = 7
INNER = 9
AXES = ("mem", "lat", "lon")
MASKED = -1e30
EXP2_SCALE = math.log2(math.e) / math.sqrt(HDIM)
BF16 = jnp.bfloat16
F32 = jnp.float32
NT = (((1,), (1,)), ((), ()))

eps = 1e-05


def place(j):
    return j & 3, ((j >> 2) & 1) * 2 + ((j >> 6) & 1), (j >> 3) & 3, (j >> 5) & 1


def flat(x, y, z, core):
    return ((y & 1) << 6) | (core << 5) | (z << 3) | ((y >> 1) << 2) | x


def send(block, source_of):
    pairs = [(flat(*source_of(*place(j))), j) for j in range(128)]
    return lax.ppermute(block, AXES, pairs)


def along_x(block, d):
    return send(block, lambda x, y, z, c: ((x + d) % 4, y, z, c))


def along_first(block, d):
    return send(block, lambda x, y, z, c: (x, (y + d * (1 - c)) % 4, (z + d * c) % 4, c))


def along_second(block, d):
    return send(block, lambda x, y, z, c: (x, (y + d * c) % 4, (z + d * (1 - c)) % 4, c))


def other_core(block):
    return send(block, lambda x, y, z, c: (x, y, z, 1 - c))


def from_grid(block, dlat, dlon):
    pairs = []
    for j in range(128):
        mem, lat, lon = j >> 5, (j >> 3) & 3, j & 7
        pairs.append((mem * 32 + ((lat + dlat) % 4) * 8 + (lon + dlon) % 8, j))
    return lax.ppermute(block, AXES, pairs)


def norm(values, gain):
    average = jnp.mean(values, axis=-1, keepdims=True)
    centred = values - average
    variance = jnp.mean(centred * centred, axis=-1, keepdims=True)
    return (centred * lax.rsqrt(variance + eps) * gain).astype(BF16)


def prep_kernel(ext_ref, ids_ref, gain_ref, f_ref, x_ref, xq_ref, bias_ref):
    i = pl.program_id(0)
    k = i - EDGE
    wi = jnp.where(i < 4, 3, jnp.where(i < EDGE, i - 4, k // 3))
    wj = jnp.where(i < 4, i, jnp.where(i < EDGE, 3, k % 3))
    base = jnp.where(wj < 2, 0, jnp.where(wj == 2, 16, 32))
    off = 12 * wj + SL - base
    col = lax.broadcasted_iota(jnp.int32, (1, 384), 1)
    seg = col // 32
    cc = col - seg * 32 - off
    lev = (seg >= 6).astype(jnp.int32)
    r = seg - 6 * lev
    rh = (r >= 3).astype(jnp.int32)
    ch = (cc >= 6).astype(jnp.int32)
    quad = jnp.where(wj == 3, ch * 2 + rh, rh * 2 + ch)
    row = quad * 36 + lev * 18 + (r - 3 * rh) * 6 + cc - 6 * ch
    row = jnp.where((cc >= 0) & (cc < 12), row, -1)
    pick = (lax.broadcasted_iota(jnp.int32, (TOK, 384), 0) == row).astype(F32).astype(BF16)
    start = pl.multiple_of(base, 16)
    tokens = jnp.concatenate(
        [ext_ref[s // 6, 6 * wi + SH + s % 6, pl.ds(start, 32), :] for s in range(12)], axis=0
    )
    marks = jnp.concatenate([ids_ref[6 * wi + SH + s % 6, pl.ds(start, 32), :] for s in range(12)], axis=0)
    f = jnp.dot(pick, tokens, preferred_element_type=F32)
    idk = jnp.dot(pick, marks, preferred_element_type=F32)
    f_ref[0] = f.astype(BF16)
    x = norm(f, gain_ref[...])
    x_ref[0] = x
    xq_ref[0, 0:128] = x[0:128]
    for t in range(8):
        xq_ref[0, 128 + 16 * t : 144 + 16 * t] = x[128:144]
    idq = jnp.concatenate([idk[0:128]] + [idk[128:144]] * 8, axis=0).T[0:1]
    both = jnp.concatenate([idk, idk], axis=1)
    bias_ref[0] = jnp.where(both == idq, 0.0, MASKED).astype(BF16)


def prep(ext, ids, gain):
    n = EDGE + INNER
    whole = lambda a: pl.BlockSpec(a.shape, lambda i: (0,) * a.ndim)
    out = lambda *s: (jax.ShapeDtypeStruct((n, *s), BF16), pl.BlockSpec((1, *s), lambda i: (i, 0, 0)))
    shapes, specs = zip(out(TOK, D), out(TOK, D), out(256, D), out(TOK, 256))
    return pl.pallas_call(
        prep_kernel,
        grid=(n,),
        in_specs=[whole(ext), whole(ids), whole(gain)],
        out_specs=specs,
        out_shape=shapes,
        name="prep",
        cost_estimate=pl.CostEstimate(flops=3_000_000_000, bytes_accessed=16_000_000, transcendentals=0),
    )(ext, ids, gain)


def block_rows(pos_ref, side, d2, d3):
    core = pos_ref[2]
    core = core if side == 0 else 1 - core
    dy = jnp.where(core == 0, d2, d3)
    dz = jnp.where(core == 0, d3, d2)
    y = (pos_ref[0] + dy) % 4
    z = (pos_ref[1] + dz) % 4
    return (y % 2) * 16 + core * 8 + z * 2 + y // 2


def attn_kernel(count, pos_ref, x_ref, xq_ref, bias_ref, *refs):
    pieces, out_ref, (w, kall, qt, vt, mt) = refs[:8], refs[8], refs[9:]
    i = pl.program_id(0)

    @pl.when(i == 0)
    def _():
        for p in range(8):
            for d2 in range(4):
                b = block_rows(pos_ref, p // 4, d2, p % 4)
                w[pl.ds(pl.multiple_of(b * 48, 16), 48), :] = pieces[p][d2]
        keys = lax.dot_general(
            x_ref[...].reshape(count * TOK, D), w[D : 2 * D, :], NT, preferred_element_type=F32
        )
        kall[...] = keys.astype(BF16)

    xq = xq_ref[0]
    qt[...] = lax.dot_general(w[0:D, :], xq, NT, preferred_element_type=F32).astype(BF16)
    vt[...] = lax.dot_general(w[2 * D : 3 * D, :], xq, NT, preferred_element_type=F32).astype(BF16)
    krow = pl.multiple_of(i * TOK, 16)
    ones = jnp.ones((16, TOK), BF16)
    bias = bias_ref[0].astype(F32)

    def soften(s):
        m = jnp.max(s, axis=0, keepdims=True)
        return jnp.exp2((s - m) * EXP2_SCALE).astype(BF16)

    for g in range(4):
        zeros = jnp.zeros((32, 128), BF16)
        heads = []
        for h in range(4):
            q = qt[128 * g + 32 * h : 128 * g + 32 * h + 32, 0:128]
            heads.append(jnp.concatenate([zeros] * h + [q] + [zeros] * (3 - h), axis=0))
        kg = kall[pl.ds(krow, TOK), 128 * g : 128 * g + 128]
        for pair in range(2):
            s = jnp.dot(
                kg, jnp.concatenate(heads[2 * pair : 2 * pair + 2], axis=1), preferred_element_type=F32
            )
            s = s + jnp.concatenate([bias[:, 0:128]] * 2, axis=1)
            p = soften(s)
            at = 128 * g + 64 * pair
            lhs = jnp.concatenate([vt[at : at + 64, 0:TOK], ones], axis=0)
            o = jnp.dot(lhs, p, preferred_element_type=F32)
            inv = 1.0 / o[64:65]
            mt[at : at + 32, 0:128] = o[0:32, 0:128] * inv[:, 0:128]
            mt[at + 32 : at + 64, 0:128] = o[32:64, 128:256] * inv[:, 128:256]
    own = (
        lax.broadcasted_iota(jnp.int32, (256, 128), 0) // 32
        == lax.broadcasted_iota(jnp.int32, (256, 128), 1) // 16
    )
    fold = (
        lax.broadcasted_iota(jnp.int32, (128, 128), 0) % 16 == lax.broadcasted_iota(jnp.int32, (128, 128), 1)
    ).astype(F32).astype(BF16)
    for a in range(2):
        q = jnp.where(own, qt[256 * a : 256 * a + 256, 128:256].astype(F32), 0.0).astype(BF16)
        s = jnp.dot(kall[pl.ds(krow, TOK), 256 * a : 256 * a + 256], q, preferred_element_type=F32)
        p = soften(s + bias[:, 128:256])
        lhs = jnp.concatenate([vt[256 * a : 256 * a + 256, 0:TOK], ones], axis=0)
        o = jnp.dot(lhs, p, preferred_element_type=F32)
        o = jnp.where(own, o[0:256] * (1.0 / o[256:257]), 0.0).astype(BF16)
        mt[256 * a : 256 * a + 256, 128:256] = jnp.dot(o, fold, preferred_element_type=F32)
    out_ref[0] = mt[...].T[0:TOK].astype(BF16)


def attend(pos, x, xq, bias, pieces, first, count):
    whole = lambda a: pl.BlockSpec(a.shape, lambda i: (0,) * a.ndim, pipeline_mode=pl.Buffered(1))
    one = lambda *s: pl.BlockSpec((1, *s), lambda i: (i + first, 0, 0))
    return pl.pallas_call(
        functools.partial(attn_kernel, count),
        grid=(count,),
        in_specs=[
            pl.BlockSpec(memory_space=pltpu.SMEM),
            whole(x),
            one(256, D),
            one(TOK, 256),
            *[whole(p) for p in pieces],
        ],
        out_specs=pl.BlockSpec((1, TOK, D), lambda i: (i, 0, 0)),
        out_shape=jax.ShapeDtypeStruct((count, TOK, D), BF16),
        scratch_shapes=[
            pltpu.VMEM((3 * D, D), BF16),
            pltpu.VMEM((count * TOK, D), BF16),
            pltpu.VMEM((D, 256), BF16),
            pltpu.VMEM((D, 256), BF16),
            pltpu.VMEM((D, 256), F32),
        ],
        name=f"attend_{first}",
        cost_estimate=pl.CostEstimate(
            flops=count * 1_000_000_000, bytes_accessed=count * 600_000, transcendentals=count * 400_000
        ),
    )(pos, x, xq, bias, *pieces)


def mlp_kernel(pos_ref, mixed_ref, f_ref, gain_ref, *refs):
    pieces, out_ref, (wp, wu, wd) = refs[:8], refs[8], refs[9:]

    @pl.when(pl.program_id(0) == 0)
    def _():
        for p in range(8):
            for d2 in range(4):
                b = block_rows(pos_ref, p // 4, d2, p % 4)
                wp[pl.ds(pl.multiple_of(b * 16, 16), 16), :] = pieces[p][d2, 0:16]
                wu[pl.ds(pl.multiple_of(b * 64, 16), 64), :] = pieces[p][d2, 16:80]
                for c in range(4):
                    wd[c, pl.ds(pl.multiple_of(b * 16, 16), 16), :] = pieces[p][d2, 80 + 16 * c : 96 + 16 * c]

    attn = lax.dot_general(mixed_ref[...], wp[...], NT, preferred_element_type=F32).astype(BF16)
    resid = (f_ref[...].astype(F32) + attn.astype(F32)).astype(BF16)
    normed = norm(resid.astype(F32), gain_ref[...])
    total = resid.astype(F32)
    for c in range(4):
        pre = lax.dot_general(normed, wu[512 * c : 512 * c + 512, :], NT, preferred_element_type=F32)
        hidden = (0.5 * pre * (1.0 + lax.erf(pre * math.sqrt(0.5)))).astype(BF16)
        total = total + lax.dot_general(hidden, wd[c], NT, preferred_element_type=F32)
    out_ref[...] = total.astype(BF16)


def mlp(pos, mixed, f, gain, pieces, first, rows, tile):
    whole = lambda a: pl.BlockSpec(a.shape, lambda i: (0,) * a.ndim, pipeline_mode=pl.Buffered(1))
    return pl.pallas_call(
        mlp_kernel,
        grid=(rows // tile,),
        in_specs=[
            pl.BlockSpec(memory_space=pltpu.SMEM),
            pl.BlockSpec((tile, D), lambda i: (i, 0)),
            pl.BlockSpec((pl.Element(tile), pl.Element(D)), lambda i: (pl.multiple_of(first + i * tile, 16), 0)),
            whole(gain),
            *[whole(p) for p in pieces],
        ],
        out_specs=pl.BlockSpec((tile, D), lambda i: (i, 0)),
        out_shape=jax.ShapeDtypeStruct((rows, D), BF16),
        scratch_shapes=[
            pltpu.VMEM((D, D), BF16),
            pltpu.VMEM((FF, D), BF16),
            pltpu.VMEM((4, D, D), BF16),
        ],
        name=f"mlp_{first}",
        cost_estimate=pl.CostEstimate(
            flops=rows * 5_000_000, bytes_accessed=rows * 3072 + 5_000_000, transcendentals=rows * 2048
        ),
    )(pos, mixed, f, gain, *pieces)


def place_matrices():
    top = np.zeros((288, 368), np.float32)
    mid = np.zeros((576, 656), np.float32)
    for lev in range(2):
        for rr in range(3):
            for c in range(48):
                o = lev * 144 + rr * 48 + c
                at = lev * 18 + rr * 6
                wj, cc = (c - 6) // 12, (c - 6) % 12
                ch, c1 = cc // 6, cc % 6
                if c < 6:
                    top[o, 320 + 12 + at + c] = 1
                    for rh in range(2):
                        mid[rh * 288 + o, 576 + 8 + 36 * rh + at + c] = 1
                elif wj < 3:
                    top[o, 80 * wj + 8 + 36 * ch + at + c1] = 1
                    for rh in range(2):
                        mid[rh * 288 + o, 144 * wj + 72 * rh + 36 * ch + at + c1] = 1
                else:
                    top[o, 240 + 4 + at + c1] = 1
                    for rh in range(2):
                        mid[rh * 288 + o, 432 + 36 * rh + at + c1] = 1
    return top, mid


def place_kernel(edge_ref, inner_ref, lat_ref, lon_ref, diag_ref, top_ref, mid_ref, out_ref):
    def put(k, rows):
        for lev in range(2):
            for rr in range(3):
                at = lev * 144 + rr * 48
                out_ref[0, lev, 3 * k + rr] = rows[at : at + 48].astype(BF16)

    first = jnp.concatenate([lat_ref[...], diag_ref[...]], axis=0)
    put(0, jnp.dot(top_ref[...], first, preferred_element_type=F32))
    for wi in range(4):
        if wi < 3:
            three = inner_ref[432 * wi : 432 * wi + 432]
            last = edge_ref[576 + 144 * wi : 720 + 144 * wi]
        else:
            three = edge_ref[0:432]
            last = edge_ref[432:576]
        stack = jnp.concatenate([three, last, lon_ref[80 * wi : 80 * wi + 80]], axis=0)
        both = 576 if wi < 3 else 288
        rows = jnp.dot(mid_ref[0:both], stack, preferred_element_type=F32)
        put(1 + 2 * wi, rows[0:288])
        if wi < 3:
            put(2 + 2 * wi, rows[288:576])


def to_grid(edge, inner, lat, lon, diag):
    top, mid = place_matrices()
    return pl.pallas_call(
        place_kernel,
        out_shape=jax.ShapeDtypeStruct((1, 2, 24, 48, D), BF16),
        name="to_grid",
        cost_estimate=pl.CostEstimate(flops=3_000_000_000, bytes_accessed=8_000_000, transcendentals=0),
    )(edge, inner, lat, lon, diag, jnp.asarray(top, BF16), jnp.asarray(mid, BF16))


def widen(own, stage):
    return jnp.stack([own, *[stage(own, d) for d in (1, 2, 3)]])


def pieces_of(block):
    group = widen(block, along_first)
    mine = [group, *[along_second(group, d) for d in (1, 2, 3)]]
    return mine + [other_core(m) for m in mine]


def body(fields, region, gain_attn, w_qkv, w_proj, gain_mlp, w_up, w_down):
    lat, lon = lax.axis_index("lat"), lax.axis_index("lon")
    mem = lax.axis_index("mem")
    pos = jnp.stack([(lon // 4) * 2 + mem // 2, lat, mem % 2]).astype(jnp.int32)

    down = w_down.T.reshape(4, 4, D).transpose(1, 0, 2).reshape(16, D)
    block = jnp.concatenate([w_qkv.T, w_proj.T, w_up.T, down], axis=0)
    line = widen(block, along_x)
    line = lax.dynamic_slice_in_dim(jnp.concatenate([line, line]), (4 - lon % 4) % 4, 4)
    qkv_pieces = pieces_of(line[:, 0:12].reshape(48, D))
    rest = jnp.concatenate(
        [
            line[:, 12:16].reshape(16, D),
            line[:, 16:32].reshape(64, D),
            line[:, 32:48].reshape(4, 4, 4, D).transpose(1, 0, 2, 3).reshape(64, D),
        ]
    )
    rest_pieces = pieces_of(rest)

    member = fields[0]
    levels, clat, clon, _ = member.shape
    row = lax.broadcasted_iota(jnp.int32, (clat, clon), 0)
    ids = (region * 2 + ((lat == 0) & (row < SH)).astype(jnp.int32)).astype(BF16)
    below = from_grid(member[:, :SH], 1, 0)
    right = from_grid(member[:, :, :SL], 0, 1)
    corner = from_grid(member[:, :SH, :SL], 1, 1)
    ids_below = from_grid(ids[:SH], 1, 0)
    ids_right = from_grid(ids[:, :SL], 0, 1)
    ids_corner = from_grid(ids[:SH, :SL], 1, 1)
    gap = jnp.zeros((levels, clat + SH, 64 - clon - SL, D), BF16)
    ext = jnp.concatenate(
        [
            jnp.concatenate([member, below], axis=1),
            jnp.concatenate([right, corner], axis=1),
            gap,
        ],
        axis=2,
    )
    ids = jnp.concatenate(
        [jnp.concatenate([ids, ids_below], axis=0), jnp.concatenate([ids_right, ids_corner], axis=0)], axis=1
    )
    ids = jnp.pad(ids, ((0, 0), (0, 64 - clon - SL)))
    ids = jnp.broadcast_to(ids[:, :, None], (clat + SH, 64, 128))
    f, x, xq, bias = prep(ext, ids, gain_attn.reshape(1, D))

    mixed_edge = attend(pos, x[:EDGE], xq, bias, qkv_pieces, 0, EDGE)
    mixed_inner = attend(pos, x[EDGE:], xq, bias, qkv_pieces, EDGE, INNER)
    f = f.reshape(-1, D)
    gain = gain_mlp.reshape(1, D)
    edge = mlp(pos, mixed_edge.reshape(-1, D), f, gain, rest_pieces, 0, EDGE * TOK, 336)
    win = edge.reshape(EDGE, TOK, D)
    lat_out = jnp.concatenate([win[0:3, 64:144].reshape(240, D), win[3, 32:112]])
    lon_out = jnp.concatenate([win[4:7, 64:144].reshape(240, D), win[3, 64:144]])
    diag_out = win[3, 96:144]
    lat_in = from_grid(lat_out, -1, 0)
    lon_in = from_grid(lon_out, 0, -1)
    diag_in = from_grid(diag_out, -1, -1)
    inner = mlp(pos, mixed_inner.reshape(-1, D), f, gain, rest_pieces, EDGE * TOK, INNER * TOK, 432)
    return to_grid(edge, inner, lat_in, lon_in, diag_in)


def solution(mesh):
    weight = P(None, AXES)
    in_specs = (
        P("mem", None, "lat", "lon", None),
        P("lat", "lon"),
        P(),
        weight,
        weight,
        P(),
        weight,
        weight,
    )
    out_specs = P("mem", None, "lat", "lon", None)
    return jax.shard_map(body, mesh=mesh, in_specs=in_specs, out_specs=out_specs, check_vma=False)
```

```python
import functools
import math

import jax
import jax.numpy as jnp
import numpy as np
from jax import lax
from jax.experimental import pallas as pl
from jax.experimental.pallas import tpu as pltpu
from jax.sharding import PartitionSpec as P

D = 512
HDIM = 32
FF = 2048
SH = 3
SL = 6
TOK = 144
EDGE = 7
INNER = 9
AXES = ("mem", "lat", "lon")
MASKED = -1e30
EXP2_SCALE = math.log2(math.e) / math.sqrt(HDIM)
BF16 = jnp.bfloat16
F32 = jnp.float32
NT = (((1,), (1,)), ((), ()))

eps = 1e-05


def place(j):
    return j & 3, ((j >> 2) & 1) * 2 + ((j >> 6) & 1), (j >> 3) & 3, (j >> 5) & 1


def flat(x, y, z, core):
    return ((y & 1) << 6) | (core << 5) | (z << 3) | ((y >> 1) << 2) | x


def send(block, source_of):
    pairs = [(flat(*source_of(*place(j))), j) for j in range(128)]
    return lax.ppermute(block, AXES, pairs)


def along_x(block, d):
    return send(block, lambda x, y, z, c: ((x + d) % 4, y, z, c))


def along_first(block, d):
    return send(block, lambda x, y, z, c: (x, (y + d * (1 - c)) % 4, (z + d * c) % 4, c))


def along_second(block, d):
    return send(block, lambda x, y, z, c: (x, (y + d * c) % 4, (z + d * (1 - c)) % 4, c))


def other_core(block):
    return send(block, lambda x, y, z, c: (x, y, z, 1 - c))


def from_grid(block, dlat, dlon):
    pairs = []
    for j in range(128):
        mem, lat, lon = j >> 5, (j >> 3) & 3, j & 7
        pairs.append((mem * 32 + ((lat + dlat) % 4) * 8 + (lon + dlon) % 8, j))
    return lax.ppermute(block, AXES, pairs)


def norm(values, gain):
    average = jnp.mean(values, axis=-1, keepdims=True)
    centred = values - average
    variance = jnp.mean(centred * centred, axis=-1, keepdims=True)
    return (centred * lax.rsqrt(variance + eps) * gain).astype(BF16)


def prep_kernel(member_ref, rows_ref, cols_ref, both_ref, ids_ref, gain_ref, f_ref, x_ref, xq_ref, bias_ref, ext, near_ref):
    step = pl.program_id(0)

    @pl.when(step == 0)
    def _():
        ext[:, 0:24, 0:48] = member_ref[...]
        for lev in range(2):
            for n in range(24):
                at = (24 * lev + n) * 8
                ext[lev, n, 48:56] = cols_ref[at : at + 8]
            for n in range(3):
                at = 3 * lev + n
                ext[lev, 24 + n, 0:48] = rows_ref[48 * at : 48 * at + 48]
                ext[lev, 24 + n, 48:56] = both_ref[8 * at : 8 * at + 8]
        ext[:, :, 56:64] = jnp.zeros((2, 27, 8, D), BF16)
        ids = ids_ref[...].astype(F32)
        for ref, at in ((rows_ref, 288), (cols_ref, 384), (both_ref, 48)):
            ids = ids + ref[at : at + 32, 0:128].astype(F32)
        near_ref[...] = jnp.concatenate([ids, jnp.zeros((96, 128), F32)], axis=0).T

    col = lax.broadcasted_iota(jnp.int32, (1, 384), 1)
    seg = col // 32
    lev = (seg >= 6).astype(jnp.int32)
    r = seg - 6 * lev
    rh = (r >= 3).astype(jnp.int32)
    lane = lax.broadcasted_iota(jnp.int32, (32, 128), 1)
    every = jnp.ones((128, 128), BF16)
    for at in range(4):
        i = 4 * step + at
        k = i - EDGE
        wi = jnp.where(i < 4, 3, jnp.where(i < EDGE, i - 4, k // 3))
        wj = jnp.where(i < 4, i, jnp.where(i < EDGE, 3, k % 3))
        base = jnp.where(wj < 2, 0, jnp.where(wj == 2, 16, 32))
        cc = col - seg * 32 - (12 * wj + SL - base)
        ch = (cc >= 6).astype(jnp.int32)
        quad = jnp.where(wj == 3, ch * 2 + rh, rh * 2 + ch)
        row = quad * 36 + lev * 18 + (r - 3 * rh) * 6 + cc - 6 * ch
        row = jnp.where((cc >= 0) & (cc < 12), row, -1)
        pick = (lax.broadcasted_iota(jnp.int32, (TOK, 384), 0) == row).astype(F32).astype(BF16)
        start = pl.multiple_of(base, 16)
        tokens = jnp.concatenate(
            [ext[n // 6, 6 * wi + SH + n % 6, pl.ds(start, 32), :] for n in range(12)], axis=0
        )
        f = jnp.dot(pick, tokens, preferred_element_type=F32)
        f_ref[at] = f.astype(BF16)
        x = norm(f, gain_ref[...])
        x_ref[at] = x
        xq_ref[at, 0:128] = x[0:128]
        for t in range(8):
            xq_ref[at, 128 + 16 * t : 144 + 16 * t] = x[128:144]
        near = near_ref[pl.ds(start, 32), :]
        marks = [jnp.where(lane == 6 * wi + SH + n, near, 0.0).astype(BF16) for n in range(6)]
        marks = jnp.dot(pick, jnp.concatenate(marks * 2, axis=0), preferred_element_type=F32)
        idk = jnp.dot(marks.astype(BF16), every, preferred_element_type=F32)
        idq = jnp.concatenate([idk[0:128]] + [idk[128:144]] * 8, axis=0).T[0:1]
        bias_ref[at] = jnp.where(jnp.concatenate([idk, idk], axis=1) == idq, 0.0, MASKED).astype(BF16)


def prep(*operands):
    n = EDGE + INNER
    whole = lambda a: pl.BlockSpec(a.shape, lambda i: (0,) * a.ndim, pipeline_mode=pl.Buffered(1))
    out = lambda *s: (jax.ShapeDtypeStruct((n, *s), BF16), pl.BlockSpec((4, *s), lambda i: (i, 0, 0)))
    shapes, specs = zip(out(TOK, D), out(TOK, D), out(256, D), out(TOK, 256))
    return pl.pallas_call(
        prep_kernel,
        grid=(n // 4,),
        in_specs=[whole(a) for a in operands],
        out_specs=specs,
        out_shape=shapes,
        scratch_shapes=[pltpu.VMEM((2, 27, 64, D), BF16), pltpu.VMEM((128, 128), F32)],
        name="prep",
        cost_estimate=pl.CostEstimate(flops=6_000_000_000, bytes_accessed=16_000_000, transcendentals=0),
    )(*operands)


def block_rows(pos_ref, side, d2, d3):
    core = pos_ref[2]
    core = core if side == 0 else 1 - core
    dy = jnp.where(core == 0, d2, d3)
    dz = jnp.where(core == 0, d3, d2)
    y = (pos_ref[0] + dy) % 4
    z = (pos_ref[1] + dz) % 4
    return (y % 2) * 16 + core * 8 + z * 2 + y // 2


def attn_kernel(pos_ref, x_ref, xq_a, xq_b, xv_a, xv_b, bias_ref, *refs):
    pieces, out_ref = refs[:2], refs[2]
    w, kall, own = refs[3:6]
    q2, v2, s2, p2, m2 = (refs[n : n + 2] for n in range(6, 16, 2))
    i = pl.program_id(0)

    @pl.when(i == 0)
    def _():
        for p in range(8):
            for d2 in range(4):
                b = block_rows(pos_ref, p // 4, d2, p % 4)
                w[pl.ds(pl.multiple_of(b * 48, 16), 48), :] = pieces[p // 4][p % 4, d2]
        keys = lax.dot_general(x_ref[...], w[D : 2 * D, :], NT, preferred_element_type=F32)
        kall[...] = keys.astype(BF16)
        own[...] = (
            lax.broadcasted_iota(jnp.int32, (256, 128), 0) // 32
            == lax.broadcasted_iota(jnp.int32, (256, 128), 1) // 16
        ).astype(F32).astype(BF16)

    ones = jnp.ones((16, TOK), BF16)
    zeros = jnp.zeros((32, 128), BF16)

    def project(dst, x, first, n):
        at = 256 * n
        out = lax.dot_general(w[first + at : first + at + 256, :], x[0], NT, preferred_element_type=F32)
        dst[at : at + 256] = out.astype(BF16)

    def scores(qt, s, krow, n):
        if n < 8:
            g = n // 2
            heads = []
            for h in (2 * (n % 2), 2 * (n % 2) + 1):
                q = qt[128 * g + 32 * h : 128 * g + 32 * h + 32, 0:128]
                heads.append(jnp.concatenate([zeros] * h + [q] + [zeros] * (3 - h), axis=0))
            kg = kall[pl.ds(krow, TOK), 128 * g : 128 * g + 128]
            s[:, 256 * n : 256 * n + 256] = jnp.dot(
                kg, jnp.concatenate(heads, axis=1), preferred_element_type=F32
            )
        else:
            for a in range(2):
                q = qt[256 * a : 256 * a + 256, 128:256] * own[...]
                s[:, 2048 + 128 * a : 2176 + 128 * a] = jnp.dot(
                    kall[pl.ds(krow, TOK), 256 * a : 256 * a + 256], q, preferred_element_type=F32
                )

    def soften(s, p, win, n):
        side = 0 if n < 8 else 128
        bias = bias_ref[win, :, side : side + 128].astype(F32)
        for at in (256 * n, 256 * n + 128):
            v = s[:, at : at + 128] + bias
            m = jnp.max(v, axis=0, keepdims=True)
            p[:, at : at + 128] = jnp.exp2((v - m) * EXP2_SCALE).astype(BF16)

    def mix(vt, p, mt, n):
        at = 64 * n
        if n < 8:
            lhs = jnp.concatenate([vt[at : at + 64, 0:TOK], ones], axis=0)
            o = jnp.dot(lhs, p[:, 256 * n : 256 * n + 256], preferred_element_type=F32)
            inv = 1.0 / o[64:65]
            mt[at : at + 32, 0:128] = o[0:32, 0:128] * inv[:, 0:128]
            mt[at + 32 : at + 64, 0:128] = o[32:64, 128:256] * inv[:, 128:256]
        else:
            lhs = jnp.concatenate([vt[:, 0:TOK], ones], axis=0)
            o = jnp.dot(lhs, p[:, 2048:2304], preferred_element_type=F32)
            inv = 1.0 / o[D : D + 1]
            for h in range(16):
                side = 128 * (h // 8)
                part = o[32 * h : 32 * h + 32, side : side + 128] * inv[:, side : side + 128]
                mt[32 * h : 32 * h + 32, 128:256] = pltpu.roll(part, (128 - 16 * (h % 8)) % 128, 1)

    def half(par, win, xq, xv):
        new, old = par, 1 - par
        krow = pl.multiple_of(jnp.clip(win - 1, 0, 15) * TOK, 16)
        soft = jnp.clip(win - 2, 0, 15)
        for n in range(9):
            if n < 2:
                project(q2[new], xq, 0, n)
            elif n < 4:
                project(v2[new], xv, 2 * D, n - 2)
            scores(q2[old], s2[old], krow, n)
            soften(s2[new], p2[new], soft, n)
            mix(v2[old], p2[old], m2[old], n)
        out_ref[old] = m2[old][...].T[0:TOK].astype(BF16)

    half(1, 2 * i - 1, xq_a, xv_a)
    half(0, 2 * i, xq_b, xv_b)


def attend(pos, x, xq, bias, pieces):
    whole = lambda a: pl.BlockSpec(a.shape, lambda i: (0,) * a.ndim, pipeline_mode=pl.Buffered(1))
    one = lambda d: pl.BlockSpec((1, 256, D), lambda i: (jnp.clip(2 * i + d, 0, 15), 0, 0))
    return pl.pallas_call(
        attn_kernel,
        grid=(10,),
        in_specs=[
            pl.BlockSpec(memory_space=pltpu.SMEM),
            whole(x),
            one(-1),
            one(0),
            one(-3),
            one(-2),
            whole(bias),
            *[whole(p) for p in pieces],
        ],
        out_specs=pl.BlockSpec((2, TOK, D), lambda i: (jnp.clip(i - 2, 0, 7), 0, 0)),
        out_shape=jax.ShapeDtypeStruct((16, TOK, D), BF16),
        scratch_shapes=[
            pltpu.VMEM((3 * D, D), BF16),
            pltpu.VMEM((16 * TOK, D), BF16),
            pltpu.VMEM((256, 128), BF16),
            *[pltpu.VMEM((D, 256), BF16)] * 4,
            *[pltpu.VMEM((TOK, 2304), F32)] * 2,
            *[pltpu.VMEM((TOK, 2304), BF16)] * 2,
            *[pltpu.VMEM((D, 256), F32)] * 2,
        ],
        name="attend",
        cost_estimate=pl.CostEstimate(flops=20_000_000_000, bytes_accessed=12_000_000, transcendentals=5_000_000),
    )(pos, x, xq, xq, xq, xq, bias, *pieces)


def mlp_kernel(pos_ref, mixed_ref, f_ref, gain_ref, *refs):
    pieces, out_ref, (wp, wu, wd, held, normed) = refs[:8], refs[8], refs[9:]

    @pl.when(pl.program_id(0) == 0)
    def _():
        for d3 in range(4):
            for d2 in range(4):
                for side in range(2):
                    b = block_rows(pos_ref, side, d2, d3)
                    piece = pieces[4 * side + d3].at[d2]
                    wp[pl.ds(pl.multiple_of(b * 16, 16), 16), :] = piece[0:16]
                    wu[pl.ds(pl.multiple_of(b * 64, 16), 64), :] = piece[16:80]
                    for c in range(4):
                        wd[c, pl.ds(pl.multiple_of(b * 16, 16), 16), :] = piece[80 + 16 * c : 96 + 16 * c]

    rows = out_ref.shape[0]
    sub = rows // 2

    def first(j):
        r = slice(j * sub, (j + 1) * sub)
        attn = lax.dot_general(mixed_ref[r], wp[...], NT, preferred_element_type=F32).astype(BF16)
        resid = (f_ref[r].astype(F32) + attn.astype(F32)).astype(BF16)
        held[r] = resid
        normed[r] = norm(resid.astype(F32), gain_ref[...])

    def second(j):
        r = slice(j * sub, (j + 1) * sub)
        total = None
        for c in range(4):
            pre = lax.dot_general(normed[r], wu[512 * c : 512 * c + 512, :], NT, preferred_element_type=F32)
            hidden = (0.5 * pre * (1.0 + lax.erf(pre * math.sqrt(0.5)))).astype(BF16)
            part = lax.dot_general(hidden, wd[c], NT, preferred_element_type=F32)
            total = part if total is None else total + part
        out_ref[r] = (held[r].astype(F32) + total).astype(BF16)

    first(0)
    first(1)
    second(0)
    second(1)


def mlp(pos, mixed, f, gain, pieces, first, rows):
    run = pl.BlockSpec((pl.Element(rows), pl.Element(D)), lambda i: (first, 0), pipeline_mode=pl.Buffered(1))
    whole = lambda a: pl.BlockSpec(a.shape, lambda i: (0,) * a.ndim, pipeline_mode=pl.Buffered(1))
    return pl.pallas_call(
        mlp_kernel,
        grid=(1,),
        in_specs=[
            pl.BlockSpec(memory_space=pltpu.SMEM),
            run,
            run,
            whole(gain),
            *[whole(p) for p in pieces],
        ],
        out_specs=pl.BlockSpec((rows, D), lambda i: (0, 0)),
        out_shape=jax.ShapeDtypeStruct((rows, D), BF16),
        scratch_shapes=[
            pltpu.VMEM((D, D), BF16),
            pltpu.VMEM((FF, D), BF16),
            pltpu.VMEM((4, D, D), BF16),
            pltpu.VMEM((rows, D), BF16),
            pltpu.VMEM((rows, D), BF16),
        ],
        name=f"mlp_{first}",
        compiler_params=pltpu.CompilerParams(vmem_limit_bytes=26 * 2**20),
        cost_estimate=pl.CostEstimate(
            flops=rows * 5_000_000, bytes_accessed=rows * 3072 + 5_000_000, transcendentals=rows * 2048
        ),
    )(pos, mixed, f, gain, *pieces)


def place_matrices():
    top = np.zeros((288, 368), np.float32)
    mid = np.zeros((576, 656), np.float32)
    for lev in range(2):
        for rr in range(3):
            for c in range(48):
                o = lev * 144 + rr * 48 + c
                at = lev * 18 + rr * 6
                wj, cc = (c - 6) // 12, (c - 6) % 12
                ch, c1 = cc // 6, cc % 6
                if c < 6:
                    top[o, 320 + 12 + at + c] = 1
                    for rh in range(2):
                        mid[rh * 288 + o, 576 + 8 + 36 * rh + at + c] = 1
                elif wj < 3:
                    top[o, 80 * wj + 8 + 36 * ch + at + c1] = 1
                    for rh in range(2):
                        mid[rh * 288 + o, 144 * wj + 72 * rh + 36 * ch + at + c1] = 1
                else:
                    top[o, 240 + 4 + at + c1] = 1
                    for rh in range(2):
                        mid[rh * 288 + o, 432 + 36 * rh + at + c1] = 1
    return top, mid


def place_kernel(edge_ref, inner_ref, lat_ref, lon_ref, diag_ref, top_ref, mid_ref, out_ref):
    def put(k, rows):
        for lev in range(2):
            for rr in range(3):
                at = lev * 144 + rr * 48
                out_ref[0, lev, 3 * k + rr] = rows[at : at + 48].astype(BF16)

    first = jnp.concatenate([lat_ref[...], diag_ref[...]], axis=0)
    put(0, jnp.dot(top_ref[...], first, preferred_element_type=F32))
    for wi in range(4):
        if wi < 3:
            three = inner_ref[432 * wi : 432 * wi + 432]
            last = edge_ref[576 + 144 * wi : 720 + 144 * wi]
        else:
            three = edge_ref[0:432]
            last = edge_ref[432:576]
        stack = jnp.concatenate([three, last, lon_ref[80 * wi : 80 * wi + 80]], axis=0)
        both = 576 if wi < 3 else 288
        rows = jnp.dot(mid_ref[0:both], stack, preferred_element_type=F32)
        put(1 + 2 * wi, rows[0:288])
        if wi < 3:
            put(2 + 2 * wi, rows[288:576])


def to_grid(edge, inner, lat, lon, diag):
    top, mid = place_matrices()
    return pl.pallas_call(
        place_kernel,
        out_shape=jax.ShapeDtypeStruct((1, 2, 24, 48, D), BF16),
        name="to_grid",
        compiler_params=pltpu.CompilerParams(vmem_limit_bytes=20 * 2**20),
        cost_estimate=pl.CostEstimate(flops=3_000_000_000, bytes_accessed=8_000_000, transcendentals=0),
    )(edge, inner, lat, lon, diag, jnp.asarray(top, BF16), jnp.asarray(mid, BF16))


def widen(own, stage):
    return jnp.stack([own, *[stage(own, d) for d in (1, 2, 3)]])


def after(value, *others):
    return lax.optimization_barrier((value, *others))[0]


def body(fields, region, gain_attn, w_qkv, w_proj, gain_mlp, w_up, w_down):
    lat, lon = lax.axis_index("lat"), lax.axis_index("lon")
    mem = lax.axis_index("mem")
    pos = jnp.stack([(lon // 4) * 2 + mem // 2, lat, mem % 2]).astype(jnp.int32)

    down = w_down.T.reshape(4, 4, D).transpose(1, 0, 2).reshape(16, D)
    block = jnp.concatenate([w_qkv.T, w_proj.T, w_up.T, down], axis=0)
    line = widen(block, along_x)
    line = lax.dynamic_slice_in_dim(jnp.concatenate([line, line]), (4 - lon % 4) % 4, 4)
    stage = jnp.concatenate(
        [
            line[:, 0:12].reshape(48, D),
            line[:, 12:16].reshape(16, D),
            line[:, 16:32].reshape(64, D),
            line[:, 32:48].reshape(4, 4, 4, D).transpose(1, 0, 2, 3).reshape(64, D),
        ]
    )

    member = fields[0]
    levels, clat, clon, _ = member.shape
    row = lax.broadcasted_iota(jnp.int32, (clat, clon), 0)
    ids = (region * 2 + ((lat == 0) & (row < SH)).astype(jnp.int32)).astype(BF16)

    def payload(part, marks, top, left):
        marks = jnp.pad(marks, ((top, 32 - top - marks.shape[0]), (left, D - left - marks.shape[1])))
        return jnp.concatenate([part.reshape(-1, D), marks])

    rows = from_grid(payload(member[:, :SH], ids[:SH], clat, 0), 1, 0)
    cols = from_grid(payload(member[:, :, :8], ids[:, :8], 0, clon), 0, 1)
    both = from_grid(payload(member[:, :SH, :8], ids[:SH, :8], clat, clon), 1, 1)
    ids = jnp.pad(ids, ((0, 32 - clat), (0, 128 - clon)))

    firsts = [along_first(stage, d) for d in (1, 2, 3)]
    f, x, xq, bias = prep(member, rows, cols, both, ids, gain_attn.reshape(1, D))
    firsts = lax.optimization_barrier((*firsts, f))[:3]
    group = jnp.stack([p[0:48] for p in (stage, *firsts)])
    rest = jnp.stack([p[48:192] for p in (stage, *firsts)])
    qkv_mine = widen(group, along_second)
    qkv_pieces = [qkv_mine, other_core(qkv_mine)]
    rest = after(rest, qkv_mine)
    rest_mine = [rest, *[along_second(rest, d) for d in (1, 2, 3)]]
    mixed = attend(pos, x.reshape(-1, D), xq, bias, qkv_pieces).reshape(-1, D)
    late = lax.optimization_barrier((*rest_mine, mixed))[:4]
    rest_pieces = [*late, *[other_core(p) for p in late]]
    f = f.reshape(-1, D)
    gain = gain_mlp.reshape(1, D)
    edge = mlp(pos, mixed, f, gain, rest_pieces, 0, EDGE * TOK)
    win = edge.reshape(EDGE, TOK, D)
    lat_out = jnp.concatenate([win[0:3, 64:144].reshape(240, D), win[3, 32:112]])
    lon_out = jnp.concatenate([win[4:7, 64:144].reshape(240, D), win[3, 64:144]])
    diag_out = win[3, 96:144]
    lat_in = from_grid(lat_out, -1, 0)
    lon_in = from_grid(lon_out, 0, -1)
    diag_in = from_grid(diag_out, -1, -1)
    inner = mlp(pos, mixed, f, gain, rest_pieces, EDGE * TOK, INNER * TOK)
    return to_grid(edge, inner, lat_in, lon_in, diag_in)


def solution(mesh):
    weight = P(None, AXES)
    in_specs = (
        P("mem", None, "lat", "lon", None),
        P("lat", "lon"),
        P(),
        weight,
        weight,
        P(),
        weight,
        weight,
    )
    out_specs = P("mem", None, "lat", "lon", None)
    return jax.shard_map(body, mesh=mesh, in_specs=in_specs, out_specs=out_specs, check_vma=False)
```

```python
import math

import jax
import jax.numpy as jnp
import numpy as np
from jax import lax
from jax.experimental import pallas as pl
from jax.experimental.pallas import tpu as pltpu
from jax.sharding import PartitionSpec as P


D = 512
HDIM = 32
FF = 2048
SH = 3
SL = 6
TOK = 144
EDGE = 7
INNER = 9
AXES = ("mem", "lat", "lon")
MASKED = -1e30
EXP2_SCALE = math.log2(math.e) / math.sqrt(HDIM)
BF16 = jnp.bfloat16
F32 = jnp.float32
NT = (((1,), (1,)), ((), ()))

eps = 1e-05


def place(j):
    return j & 3, ((j >> 2) & 1) * 2 + ((j >> 6) & 1), (j >> 3) & 3, (j >> 5) & 1


def flat(x, y, z, core):
    return ((y & 1) << 6) | (core << 5) | (z << 3) | ((y >> 1) << 2) | x


def send(block, source_of):
    pairs = [(flat(*source_of(*place(j))), j) for j in range(128)]
    return lax.ppermute(block, AXES, pairs)


def along_x(block, d):
    return send(block, lambda x, y, z, c: ((x + d) % 4, y, z, c))


def along_first(block, d):
    return send(block, lambda x, y, z, c: (x, (y + d * (1 - c)) % 4, (z + d * c) % 4, c))


def along_second(block, d):
    return send(block, lambda x, y, z, c: (x, (y + d * c) % 4, (z + d * (1 - c)) % 4, c))


def other_core(block):
    return send(block, lambda x, y, z, c: (x, y, z, 1 - c))


def from_grid(block, dlat, dlon):
    pairs = []
    for j in range(128):
        mem, lat, lon = j >> 5, (j >> 3) & 3, j & 7
        pairs.append((mem * 32 + ((lat + dlat) % 4) * 8 + (lon + dlon) % 8, j))
    return lax.ppermute(block, AXES, pairs)


def norm(values, gain):
    average = jnp.mean(values, axis=-1, keepdims=True)
    centred = values - average
    variance = jnp.mean(centred * centred, axis=-1, keepdims=True)
    return (centred * lax.rsqrt(variance + eps) * gain).astype(BF16)


def prep_kernel(member_ref, rows_ref, cols_ref, both_ref, ids_ref, gain_ref, f_ref, x_ref, xq_ref, bias_ref, ext, near_ref):
    step = pl.program_id(0)

    @pl.when(step == 0)
    def _():
        ext[:, 0:24, 0:48] = member_ref[...]
        for lev in range(2):
            for n in range(24):
                at = (24 * lev + n) * 8
                ext[lev, n, 48:56] = cols_ref[at : at + 8]
            for n in range(3):
                at = 3 * lev + n
                ext[lev, 24 + n, 0:48] = rows_ref[48 * at : 48 * at + 48]
                ext[lev, 24 + n, 48:56] = both_ref[8 * at : 8 * at + 8]
        ext[:, :, 56:64] = jnp.zeros((2, 27, 8, D), BF16)
        ids = ids_ref[...].astype(F32)
        for ref, at in ((rows_ref, 288), (cols_ref, 384), (both_ref, 48)):
            ids = ids + ref[at : at + 32, 0:128].astype(F32)
        near_ref[...] = jnp.concatenate([ids, jnp.zeros((96, 128), F32)], axis=0).T

    col = lax.broadcasted_iota(jnp.int32, (1, 384), 1)
    seg = col // 32
    lev = (seg >= 6).astype(jnp.int32)
    r = seg - 6 * lev
    rh = (r >= 3).astype(jnp.int32)
    lane = lax.broadcasted_iota(jnp.int32, (32, 128), 1)
    every = jnp.ones((128, 128), BF16)
    for at in range(4):
        i = 4 * step + at
        k = i - EDGE
        wi = jnp.where(i < 4, 3, jnp.where(i < EDGE, i - 4, k // 3))
        wj = jnp.where(i < 4, i, jnp.where(i < EDGE, 3, k % 3))
        base = jnp.where(wj < 2, 0, jnp.where(wj == 2, 16, 32))
        cc = col - seg * 32 - (12 * wj + SL - base)
        ch = (cc >= 6).astype(jnp.int32)
        quad = jnp.where(wj == 3, ch * 2 + rh, rh * 2 + ch)
        row = quad * 36 + lev * 18 + (r - 3 * rh) * 6 + cc - 6 * ch
        row = jnp.where((cc >= 0) & (cc < 12), row, -1)
        pick = (lax.broadcasted_iota(jnp.int32, (TOK, 384), 0) == row).astype(F32).astype(BF16)
        start = pl.multiple_of(base, 16)
        tokens = jnp.concatenate(
            [ext[n // 6, 6 * wi + SH + n % 6, pl.ds(start, 32), :] for n in range(12)], axis=0
        )
        f = jnp.dot(pick, tokens, preferred_element_type=F32)
        f_ref[at] = f.astype(BF16)
        x = norm(f, gain_ref[...])
        x_ref[at] = x
        xq_ref[at, 0:128] = x[0:128]
        for t in range(8):
            xq_ref[at, 128 + 16 * t : 144 + 16 * t] = x[128:144]
        near = near_ref[pl.ds(start, 32), :]
        marks = [jnp.where(lane == 6 * wi + SH + n, near, 0.0).astype(BF16) for n in range(6)]
        marks = jnp.dot(pick, jnp.concatenate(marks * 2, axis=0), preferred_element_type=F32)
        idk = jnp.dot(marks.astype(BF16), every, preferred_element_type=F32)
        idq = jnp.concatenate([idk[0:128]] + [idk[128:144]] * 8, axis=0).T[0:1]
        bias_ref[at] = jnp.where(jnp.concatenate([idk, idk], axis=1) == idq, 0.0, MASKED).astype(BF16)


def prep(*operands):
    n = EDGE + INNER
    whole = lambda a: pl.BlockSpec(a.shape, lambda i: (0,) * a.ndim, pipeline_mode=pl.Buffered(1))
    out = lambda *s: (jax.ShapeDtypeStruct((n, *s), BF16), pl.BlockSpec((4, *s), lambda i: (i, 0, 0)))
    shapes, specs = zip(out(TOK, D), out(TOK, D), out(256, D), out(TOK, 256))
    return pl.pallas_call(
        prep_kernel,
        grid=(n // 4,),
        in_specs=[whole(a) for a in operands],
        out_specs=specs,
        out_shape=shapes,
        scratch_shapes=[pltpu.VMEM((2, 27, 64, D), BF16), pltpu.VMEM((128, 128), F32)],
        name="prep",
        cost_estimate=pl.CostEstimate(flops=6_000_000_000, bytes_accessed=16_000_000, transcendentals=0),
    )(*operands)


def block_rows(pos_ref, side, d2, d3):
    core = pos_ref[2]
    core = core if side == 0 else 1 - core
    dy = jnp.where(core == 0, d2, d3)
    dz = jnp.where(core == 0, d3, d2)
    y = (pos_ref[0] + dy) % 4
    z = (pos_ref[1] + dz) % 4
    return (y % 2) * 16 + core * 8 + z * 2 + y // 2


def rest_rows(pos_ref, side, d2, d3):
    mine = pos_ref[2]
    dy = jnp.where(mine == 0, d2, d3)
    dz = jnp.where(mine == 0, d3, d2)
    y = (pos_ref[0] + dy) % 4
    z = (pos_ref[1] + dz) % 4
    return (y % 2) * 16 + (mine if side == 0 else 1 - mine) * 8 + z * 2 + y // 2


def attn_kernel(pos_ref, x_ref, xq_a, xq_b, xv_a, xv_b, bias_ref, *refs):
    pieces, out_ref = refs[:2], refs[2]
    w, kall, own = refs[3:6]
    q2, v2, s2, p2, m2 = (refs[n : n + 2] for n in range(6, 16, 2))
    i = pl.program_id(0)

    @pl.when(i == 0)
    def _():
        for p in range(8):
            for d2 in range(4):
                b = block_rows(pos_ref, p // 4, d2, p % 4)
                w[pl.ds(pl.multiple_of(b * 48, 16), 48), :] = pieces[p // 4][p % 4, d2]
        keys = lax.dot_general(x_ref[...], w[D : 2 * D, :], NT, preferred_element_type=F32)
        kall[...] = keys.astype(BF16)
        own[...] = (
            lax.broadcasted_iota(jnp.int32, (256, 128), 0) // 32
            == lax.broadcasted_iota(jnp.int32, (256, 128), 1) // 16
        ).astype(F32).astype(BF16)

    ones = jnp.ones((16, TOK), BF16)
    zeros = jnp.zeros((32, 128), BF16)

    def project(dst, x, first, n):
        at = 256 * n
        out = lax.dot_general(w[first + at : first + at + 256, :], x[0], NT, preferred_element_type=F32)
        dst[at : at + 256] = out.astype(BF16)

    def scores(qt, s, krow, n):
        if n < 8:
            g = n // 2
            heads = []
            for h in (2 * (n % 2), 2 * (n % 2) + 1):
                q = qt[128 * g + 32 * h : 128 * g + 32 * h + 32, 0:128]
                heads.append(jnp.concatenate([zeros] * h + [q] + [zeros] * (3 - h), axis=0))
            kg = kall[pl.ds(krow, TOK), 128 * g : 128 * g + 128]
            s[:, 256 * n : 256 * n + 256] = jnp.dot(
                kg, jnp.concatenate(heads, axis=1), preferred_element_type=F32
            )
        else:
            for a in range(2):
                q = qt[256 * a : 256 * a + 256, 128:256] * own[...]
                s[:, 2048 + 128 * a : 2176 + 128 * a] = jnp.dot(
                    kall[pl.ds(krow, TOK), 256 * a : 256 * a + 256], q, preferred_element_type=F32
                )

    def soften(s, p, win, n):
        side = 0 if n < 8 else 128
        bias = bias_ref[win, :, side : side + 128].astype(F32)
        for at in (256 * n, 256 * n + 128):
            v = s[:, at : at + 128] + bias
            m = jnp.max(v, axis=0, keepdims=True)
            p[:, at : at + 128] = jnp.exp2((v - m) * EXP2_SCALE).astype(BF16)

    def mix(vt, p, mt, n):
        at = 64 * n
        if n < 8:
            lhs = jnp.concatenate([vt[at : at + 64, 0:TOK], ones], axis=0)
            o = jnp.dot(lhs, p[:, 256 * n : 256 * n + 256], preferred_element_type=F32)
            inv = 1.0 / o[64:65]
            mt[at : at + 32, 0:128] = o[0:32, 0:128] * inv[:, 0:128]
            mt[at + 32 : at + 64, 0:128] = o[32:64, 128:256] * inv[:, 128:256]
        else:
            lhs = jnp.concatenate([vt[:, 0:TOK], ones], axis=0)
            o = jnp.dot(lhs, p[:, 2048:2304], preferred_element_type=F32)
            inv = 1.0 / o[D : D + 1]
            for h in range(16):
                side = 128 * (h // 8)
                part = o[32 * h : 32 * h + 32, side : side + 128] * inv[:, side : side + 128]
                mt[32 * h : 32 * h + 32, 128:256] = pltpu.roll(part, (128 - 16 * (h % 8)) % 128, 1)

    def half(par, win, xq, xv):
        new, old = par, 1 - par
        krow = pl.multiple_of(jnp.clip(win - 1, 0, 15) * TOK, 16)
        soft = jnp.clip(win - 2, 0, 15)
        for n in range(9):
            if n < 2:
                project(q2[new], xq, 0, n)
            elif n < 4:
                project(v2[new], xv, 2 * D, n - 2)
            scores(q2[old], s2[old], krow, n)
            soften(s2[new], p2[new], soft, n)
            mix(v2[old], p2[old], m2[old], n)
        out_ref[old] = m2[old][...].T[0:TOK].astype(BF16)

    half(1, 2 * i - 1, xq_a, xv_a)
    half(0, 2 * i, xq_b, xv_b)


def far(array):
    return pltpu.with_memory_space_constraint(array, pltpu.HBM)


def attend(pos, x, xq, bias, pieces):
    whole = lambda a: pl.BlockSpec(a.shape, lambda i: (0,) * a.ndim, pipeline_mode=pl.Buffered(1))
    one = lambda d: pl.BlockSpec((1, 256, D), lambda i: (jnp.clip(2 * i + d, 0, 15), 0, 0))
    return pl.pallas_call(
        attn_kernel,
        grid=(10,),
        in_specs=[
            pl.BlockSpec(memory_space=pltpu.SMEM),
            whole(x),
            one(-1),
            one(0),
            one(-3),
            one(-2),
            whole(bias),
            *[whole(p) for p in pieces],
        ],
        out_specs=pl.BlockSpec((2, TOK, D), lambda i: (jnp.clip(i - 2, 0, 7), 0, 0)),
        out_shape=jax.ShapeDtypeStruct((16, TOK, D), BF16),
        scratch_shapes=[
            pltpu.VMEM((3 * D, D), BF16),
            pltpu.VMEM((16 * TOK, D), BF16),
            pltpu.VMEM((256, 128), BF16),
            *[pltpu.VMEM((D, 256), BF16)] * 4,
            *[pltpu.VMEM((TOK, 2304), F32)] * 2,
            *[pltpu.VMEM((TOK, 2304), BF16)] * 2,
            *[pltpu.VMEM((D, 256), F32)] * 2,
        ],
        name="attend",
        compiler_params=pltpu.CompilerParams(vmem_limit_bytes=36 * 2**20),
        cost_estimate=pl.CostEstimate(flops=20_000_000_000, bytes_accessed=12_000_000, transcendentals=5_000_000),
    )(pos, far(x), *[far(xq)] * 4, far(bias), *pieces)


def mlp_kernel(pos_ref, mixed_ref, f_ref, gain_ref, *refs):
    pieces, out_ref, sent, (wp, wu, wd, held, normed) = refs[:4], refs[4], refs[5:-5], refs[-5:]

    @pl.when(pl.program_id(0) == 0)
    def _():
        for d3 in range(4):
            for d2 in range(4):
                for side in range(2):
                    b = rest_rows(pos_ref, side, d2, d3)
                    piece = pieces[d3].at[d2, side]
                    wp[pl.ds(pl.multiple_of(b * 16, 16), 16), :] = piece[0:16]
                    wu[pl.ds(pl.multiple_of(b * 64, 16), 64), :] = piece[16:80]
                    for c in range(4):
                        wd[c, pl.ds(pl.multiple_of(b * 16, 16), 16), :] = piece[80 + 16 * c : 96 + 16 * c]

    rows = out_ref.shape[0]
    sub = rows // 2

    def first(j):
        r = slice(j * sub, (j + 1) * sub)
        attn = lax.dot_general(mixed_ref[r], wp[...], NT, preferred_element_type=F32).astype(BF16)
        resid = (f_ref[r].astype(F32) + attn.astype(F32)).astype(BF16)
        held[r] = resid
        normed[r] = norm(resid.astype(F32), gain_ref[...])

    def second(j):
        r = slice(j * sub, (j + 1) * sub)
        total = None
        for c in range(4):
            pre = lax.dot_general(normed[r], wu[512 * c : 512 * c + 512, :], NT, preferred_element_type=F32)
            hidden = (0.5 * pre * (1.0 + lax.erf(pre * math.sqrt(0.5)))).astype(BF16)
            part = lax.dot_general(hidden, wd[c], NT, preferred_element_type=F32)
            total = part if total is None else total + part
        out_ref[r] = (held[r].astype(F32) + total).astype(BF16)

    first(0)
    first(1)
    second(0)
    second(1)
    if sent:
        lat_ref, lon_ref, diag_ref = sent
        corner = 3 * TOK
        for n in range(3):
            lat_ref[80 * n : 80 * n + 80] = out_ref[TOK * n + 64 : TOK * n + 144]
            lon_ref[80 * n : 80 * n + 80] = out_ref[TOK * n + 4 * TOK + 64 : TOK * n + 5 * TOK]
        lat_ref[240:320] = out_ref[corner + 32 : corner + 112]
        lon_ref[240:320] = out_ref[corner + 64 : corner + 144]
        diag_ref[...] = out_ref[corner + 96 : corner + 144]


def mlp(pos, mixed, f, gain, pieces, first, rows, sent=()):
    run = pl.BlockSpec((pl.Element(rows), pl.Element(D)), lambda i: (first, 0), pipeline_mode=pl.Buffered(1))
    whole = lambda a: pl.BlockSpec(a.shape, lambda i: (0,) * a.ndim, pipeline_mode=pl.Buffered(1))
    return pl.pallas_call(
        mlp_kernel,
        grid=(1,),
        in_specs=[
            pl.BlockSpec(memory_space=pltpu.SMEM),
            run,
            run,
            whole(gain),
            *[whole(p) for p in pieces],
        ],
        out_specs=[pl.BlockSpec((n, D), lambda i: (0, 0)) for n in (rows, *sent)],
        out_shape=[jax.ShapeDtypeStruct((n, D), BF16) for n in (rows, *sent)],
        scratch_shapes=[
            pltpu.VMEM((D, D), BF16),
            pltpu.VMEM((FF, D), BF16),
            pltpu.VMEM((4, D, D), BF16),
            pltpu.VMEM((rows, D), BF16),
            pltpu.VMEM((rows, D), BF16),
        ],
        compiler_params=pltpu.CompilerParams(vmem_limit_bytes=26 * 2**20),
        cost_estimate=pl.CostEstimate(
            flops=rows * 5_000_000, bytes_accessed=rows * 3072 + 5_000_000, transcendentals=rows * 2048
        ),
    )(pos, mixed, f, gain, *pieces)


def place_matrices():
    top = np.zeros((288, 368), np.float32)
    mid = np.zeros((576, 656), np.float32)
    for lev in range(2):
        for rr in range(3):
            for c in range(48):
                o = lev * 144 + rr * 48 + c
                at = lev * 18 + rr * 6
                wj, cc = (c - 6) // 12, (c - 6) % 12
                ch, c1 = cc // 6, cc % 6
                if c < 6:
                    top[o, 320 + 12 + at + c] = 1
                    for rh in range(2):
                        mid[rh * 288 + o, 576 + 8 + 36 * rh + at + c] = 1
                elif wj < 3:
                    top[o, 80 * wj + 8 + 36 * ch + at + c1] = 1
                    for rh in range(2):
                        mid[rh * 288 + o, 144 * wj + 72 * rh + 36 * ch + at + c1] = 1
                else:
                    top[o, 240 + 4 + at + c1] = 1
                    for rh in range(2):
                        mid[rh * 288 + o, 432 + 36 * rh + at + c1] = 1
    return top, mid


def place_kernel(edge_ref, inner_ref, lat_ref, lon_ref, diag_ref, top_ref, mid_ref, out_ref):
    def put(k, rows):
        for lev in range(2):
            for rr in range(3):
                at = lev * 144 + rr * 48
                out_ref[0, lev, 3 * k + rr] = rows[at : at + 48].astype(BF16)

    first = jnp.concatenate([lat_ref[...], diag_ref[...]], axis=0)
    put(0, jnp.dot(top_ref[...], first, preferred_element_type=F32))
    for wi in range(4):
        if wi < 3:
            three = inner_ref[432 * wi : 432 * wi + 432]
            last = edge_ref[576 + 144 * wi : 720 + 144 * wi]
        else:
            three = edge_ref[0:432]
            last = edge_ref[432:576]
        stack = jnp.concatenate([three, last, lon_ref[80 * wi : 80 * wi + 80]], axis=0)
        both = 576 if wi < 3 else 288
        rows = jnp.dot(mid_ref[0:both], stack, preferred_element_type=F32)
        put(1 + 2 * wi, rows[0:288])
        if wi < 3:
            put(2 + 2 * wi, rows[288:576])


def to_grid(edge, inner, lat, lon, diag):
    top, mid = place_matrices()
    return pl.pallas_call(
        place_kernel,
        out_shape=jax.ShapeDtypeStruct((1, 2, 24, 48, D), BF16),
        name="to_grid",
        compiler_params=pltpu.CompilerParams(vmem_limit_bytes=20 * 2**20),
        cost_estimate=pl.CostEstimate(flops=3_000_000_000, bytes_accessed=8_000_000, transcendentals=0),
    )(edge, inner, lat, lon, diag, jnp.asarray(top, BF16), jnp.asarray(mid, BF16))


def widen(own, stage):
    return jnp.stack([own, *[stage(own, d) for d in (1, 2, 3)]])


def body(fields, region, gain_attn, w_qkv, w_proj, gain_mlp, w_up, w_down):
    lat, lon = lax.axis_index("lat"), lax.axis_index("lon")
    mem = lax.axis_index("mem")
    pos = jnp.stack([(lon // 4) * 2 + mem // 2, lat, mem % 2]).astype(jnp.int32)

    down = w_down.T.reshape(4, 4, D).transpose(1, 0, 2).reshape(16, D)
    block = jnp.concatenate([w_qkv.T, w_proj.T, w_up.T, down], axis=0)
    line = widen(block, along_x)
    line = lax.dynamic_slice_in_dim(jnp.concatenate([line, line]), (4 - lon % 4) % 4, 4)
    stage = jnp.concatenate(
        [
            line[:, 0:12].reshape(48, D),
            line[:, 12:16].reshape(16, D),
            line[:, 16:32].reshape(64, D),
            line[:, 32:48].reshape(4, 4, 4, D).transpose(1, 0, 2, 3).reshape(64, D),
        ]
    )

    member = fields[0]
    _, clat, clon, _ = member.shape
    row = lax.broadcasted_iota(jnp.int32, (clat, clon), 0)
    ids = (region * 2 + ((lat == 0) & (row < SH)).astype(jnp.int32)).astype(BF16)

    def payload(part, marks, top, left):
        marks = jnp.pad(marks, ((top, 32 - top - marks.shape[0]), (left, D - left - marks.shape[1])))
        return jnp.concatenate([part.reshape(-1, D), marks])

    rows = from_grid(payload(member[:, :SH], ids[:SH], clat, 0), 1, 0)
    cols = from_grid(payload(member[:, :, :8], ids[:, :8], 0, clon), 0, 1)
    both = from_grid(payload(member[:, :SH, :8], ids[:SH, :8], clat, clon), 1, 1)
    ids = jnp.pad(ids, ((0, 32 - clat), (0, 128 - clon)))

    stage = jnp.concatenate([stage, other_core(stage[48:192])])
    firsts = [along_first(stage, d) for d in (1, 2, 3)]
    f, x, xq, bias = prep(member, rows, cols, both, ids, gain_attn.reshape(1, D))
    firsts = lax.optimization_barrier((*firsts, f))[:3]
    group = jnp.stack([p[0:48] for p in (stage, *firsts)])
    rest = jnp.stack([p[48:336].reshape(2, 144, D) for p in (stage, *firsts)])
    qkv_sent = [along_second(group, d) for d in (1, 2, 3)]
    qkv_mine = jnp.stack([group, *qkv_sent])
    qkv_pieces = [qkv_mine, other_core(qkv_mine)]
    rest_mine = [rest, *[along_second(rest, d) for d in (1, 2, 3)]]
    mixed = attend(pos, x.reshape(-1, D), xq, bias, qkv_pieces).reshape(-1, D)
    rest_pieces = lax.optimization_barrier((*rest_mine, mixed))[:4]
    f = f.reshape(-1, D)
    gain = gain_mlp.reshape(1, D)
    edge, lat_out, lon_out, diag_out = mlp(pos, mixed, f, gain, rest_pieces, 0, EDGE * TOK, (320, 320, 48))
    lat_in = from_grid(lat_out, -1, 0)
    lon_in = from_grid(lon_out, 0, -1)
    diag_in = from_grid(diag_out, -1, -1)
    (inner,) = mlp(pos, mixed, f, gain, rest_pieces, EDGE * TOK, INNER * TOK)
    return to_grid(edge, inner, lat_in, lon_in, diag_in)


def solution(mesh):
    weight = P(None, AXES)
    in_specs = (
        P("mem", None, "lat", "lon", None),
        P("lat", "lon"),
        P(),
        weight,
        weight,
        P(),
        weight,
        weight,
    )
    out_specs = P("mem", None, "lat", "lon", None)
    return jax.shard_map(body, mesh=mesh, in_specs=in_specs, out_specs=out_specs, check_vma=False)
```

```python
import math

import jax
import jax.numpy as jnp
import numpy as np
from jax import lax
from jax.experimental import pallas as pl
from jax.experimental.pallas import tpu as pltpu
from jax.sharding import PartitionSpec as P


D = 512
HDIM = 32
FF = 2048
SH = 3
SL = 6
TOK = 144
EDGE = 7
INNER = 9
AXES = ("mem", "lat", "lon")
MASKED = -1e30
EXP2_SCALE = math.log2(math.e) / math.sqrt(HDIM)
BF16 = jnp.bfloat16
F32 = jnp.float32
NT = (((1,), (1,)), ((), ()))

eps = 1e-05


def place(j):
    return j & 3, ((j >> 2) & 1) * 2 + ((j >> 6) & 1), (j >> 3) & 3, (j >> 5) & 1


def flat(x, y, z, core):
    return ((y & 1) << 6) | (core << 5) | (z << 3) | ((y >> 1) << 2) | x


def send(block, source_of):
    pairs = [(flat(*source_of(*place(j))), j) for j in range(128)]
    return lax.ppermute(block, AXES, pairs)


def along_x(block, d):
    return send(block, lambda x, y, z, c: ((x + d) % 4, y, z, c))


def along_first(block, d):
    return send(block, lambda x, y, z, c: (x, (y + d * (1 - c)) % 4, (z + d * c) % 4, c))


def along_second(block, d):
    return send(block, lambda x, y, z, c: (x, (y + d * c) % 4, (z + d * (1 - c)) % 4, c))


def other_core(block):
    return send(block, lambda x, y, z, c: (x, y, z, 1 - c))


def from_grid(block, dlat, dlon):
    pairs = []
    for j in range(128):
        mem, lat, lon = j >> 5, (j >> 3) & 3, j & 7
        pairs.append((mem * 32 + ((lat + dlat) % 4) * 8 + (lon + dlon) % 8, j))
    return lax.ppermute(block, AXES, pairs)


def norm(values, gain):
    average = jnp.mean(values, axis=-1, keepdims=True)
    centred = values - average
    variance = jnp.mean(centred * centred, axis=-1, keepdims=True)
    return (centred * lax.rsqrt(variance + eps) * gain).astype(BF16)


def prep_kernel(member_ref, rows_ref, cols_ref, both_ref, ids_ref, gain_ref, f_ref, x_ref, bias_ref, ext, near_ref):
    step = pl.program_id(0)

    @pl.when(step == 0)
    def _():
        ext[:, 0:24, 0:48] = member_ref[...]
        for lev in range(2):
            for n in range(24):
                at = (24 * lev + n) * 8
                ext[lev, n, 48:56] = cols_ref[at : at + 8]
            for n in range(3):
                at = 3 * lev + n
                ext[lev, 24 + n, 0:48] = rows_ref[48 * at : 48 * at + 48]
                ext[lev, 24 + n, 48:56] = both_ref[8 * at : 8 * at + 8]
        ext[:, :, 56:64] = jnp.zeros((2, 27, 8, D), BF16)
        ids = ids_ref[...].astype(F32)
        for ref, at in ((rows_ref, 288), (cols_ref, 384), (both_ref, 48)):
            ids = ids + ref[at : at + 32, 0:128].astype(F32)
        near_ref[...] = jnp.concatenate([ids, jnp.zeros((96, 128), F32)], axis=0).T

    col = lax.broadcasted_iota(jnp.int32, (1, 384), 1)
    seg = col // 32
    lev = (seg >= 6).astype(jnp.int32)
    r = seg - 6 * lev
    rh = (r >= 3).astype(jnp.int32)
    lane = lax.broadcasted_iota(jnp.int32, (32, 128), 1)
    every = jnp.ones((128, 128), BF16)
    for at in range(4):
        i = 4 * step + at
        k = i - EDGE
        wi = jnp.where(i < 4, 3, jnp.where(i < EDGE, i - 4, k // 3))
        wj = jnp.where(i < 4, i, jnp.where(i < EDGE, 3, k % 3))
        base = jnp.where(wj < 2, 0, jnp.where(wj == 2, 16, 32))
        cc = col - seg * 32 - (12 * wj + SL - base)
        ch = (cc >= 6).astype(jnp.int32)
        quad = jnp.where(wj == 3, ch * 2 + rh, rh * 2 + ch)
        row = quad * 36 + lev * 18 + (r - 3 * rh) * 6 + cc - 6 * ch
        row = jnp.where((cc >= 0) & (cc < 12), row, -1)
        pick = (lax.broadcasted_iota(jnp.int32, (TOK, 384), 0) == row).astype(F32).astype(BF16)
        start = pl.multiple_of(base, 16)
        tokens = jnp.concatenate(
            [ext[n // 6, 6 * wi + SH + n % 6, pl.ds(start, 32), :] for n in range(12)], axis=0
        )
        f = jnp.dot(pick, tokens, preferred_element_type=F32)
        f_ref[at] = f.astype(BF16)
        x = norm(f, gain_ref[...])
        x_ref[at] = x
        near = near_ref[pl.ds(start, 32), :]
        marks = [jnp.where(lane == 6 * wi + SH + n, near, 0.0).astype(BF16) for n in range(6)]
        marks = jnp.dot(pick, jnp.concatenate(marks * 2, axis=0), preferred_element_type=F32)
        idk = jnp.dot(marks.astype(BF16), every, preferred_element_type=F32)
        idq = jnp.concatenate([idk[0:128]] + [idk[128:144]] * 8, axis=0).T[0:1]
        bias_ref[at] = jnp.where(jnp.concatenate([idk, idk], axis=1) == idq, 0.0, MASKED).astype(BF16)


def prep(*operands):
    n = EDGE + INNER
    whole = lambda a: pl.BlockSpec(a.shape, lambda i: (0,) * a.ndim, pipeline_mode=pl.Buffered(1))
    out = lambda *s: (jax.ShapeDtypeStruct((n, *s), BF16), pl.BlockSpec((4, *s), lambda i: (i, 0, 0)))
    shapes, specs = zip(out(TOK, D), out(TOK, D), out(TOK, 256))
    return pl.pallas_call(
        prep_kernel,
        grid=(n // 4,),
        in_specs=[whole(a) for a in operands],
        out_specs=specs,
        out_shape=shapes,
        scratch_shapes=[pltpu.VMEM((2, 27, 64, D), BF16), pltpu.VMEM((128, 128), F32)],
        name="prep",
        cost_estimate=pl.CostEstimate(flops=6_000_000_000, bytes_accessed=16_000_000, transcendentals=0),
    )(*operands)


def block_rows(pos_ref, side, d2, d3):
    core = pos_ref[2]
    core = core if side == 0 else 1 - core
    dy = jnp.where(core == 0, d2, d3)
    dz = jnp.where(core == 0, d3, d2)
    y = (pos_ref[0] + dy) % 4
    z = (pos_ref[1] + dz) % 4
    return (y % 2) * 16 + core * 8 + z * 2 + y // 2


def rest_rows(pos_ref, side, d2, d3):
    mine = pos_ref[2]
    dy = jnp.where(mine == 0, d2, d3)
    dz = jnp.where(mine == 0, d3, d2)
    y = (pos_ref[0] + dy) % 4
    z = (pos_ref[1] + dz) % 4
    return (y % 2) * 16 + (mine if side == 0 else 1 - mine) * 8 + z * 2 + y // 2


def attn_kernel(pos_ref, x_ref, bias_ref, *refs):
    pieces, out_ref = refs[:2], refs[2]
    w, kall, own = refs[3:6]
    q2, v2, s2, p2, m2, x2 = (refs[n : n + 2] for n in range(6, 18, 2))
    i = pl.program_id(0)

    @pl.when(i == 0)
    def _():
        for p in range(8):
            for d2 in range(4):
                b = block_rows(pos_ref, p // 4, d2, p % 4)
                w[pl.ds(pl.multiple_of(b * 48, 16), 48), :] = pieces[p // 4][p % 4, d2]
        keys = lax.dot_general(x_ref[...], w[D : 2 * D, :], NT, preferred_element_type=F32)
        kall[...] = keys.astype(BF16)
        own[...] = (
            lax.broadcasted_iota(jnp.int32, (256, 128), 0) // 32
            == lax.broadcasted_iota(jnp.int32, (256, 128), 1) // 16
        ).astype(F32).astype(BF16)

    ones = jnp.ones((16, TOK), BF16)
    zeros = jnp.zeros((32, 128), BF16)

    def project(dst, x, first, n):
        at = 256 * n
        out = lax.dot_general(w[first + at : first + at + 256, :], x, NT, preferred_element_type=F32)
        dst[at : at + 256, 0 : x.shape[0]] = out.astype(BF16)

    def scores(qt, s, krow, n):
        if n < 8:
            g = n // 2
            heads = []
            for h in (2 * (n % 2), 2 * (n % 2) + 1):
                q = qt[128 * g + 32 * h : 128 * g + 32 * h + 32, 0:128]
                heads.append(jnp.concatenate([zeros] * h + [q] + [zeros] * (3 - h), axis=0))
            kg = kall[pl.ds(krow, TOK), 128 * g : 128 * g + 128]
            s[:, 256 * n : 256 * n + 256] = jnp.dot(
                kg, jnp.concatenate(heads, axis=1), preferred_element_type=F32
            )
        else:
            for a in range(2):
                q = qt[256 * a : 256 * a + 256, 128:256] * own[...]
                s[:, 2048 + 128 * a : 2176 + 128 * a] = jnp.dot(
                    kall[pl.ds(krow, TOK), 256 * a : 256 * a + 256], q, preferred_element_type=F32
                )

    def soften(s, p, win, n):
        side = 0 if n < 8 else 128
        bias = bias_ref[win, :, side : side + 128].astype(F32)
        for at in (256 * n, 256 * n + 128):
            v = s[:, at : at + 128] + bias
            m = jnp.max(v, axis=0, keepdims=True)
            p[:, at : at + 128] = jnp.exp2((v - m) * EXP2_SCALE).astype(BF16)

    def mix(vt, p, mt, n):
        at = 64 * n
        if n < 8:
            lhs = jnp.concatenate([vt[at : at + 64, 0:TOK], ones], axis=0)
            o = jnp.dot(lhs, p[:, 256 * n : 256 * n + 256], preferred_element_type=F32)
            inv = 1.0 / o[64:65]
            mt[at : at + 32, 0:128] = o[0:32, 0:128] * inv[:, 0:128]
            mt[at + 32 : at + 64, 0:128] = o[32:64, 128:256] * inv[:, 128:256]
        else:
            lhs = jnp.concatenate([vt[:, 0:TOK], ones], axis=0)
            o = jnp.dot(lhs, p[:, 2048:2304], preferred_element_type=F32)
            inv = 1.0 / o[D : D + 1]
            for h in range(16):
                side = 128 * (h // 8)
                part = o[32 * h : 32 * h + 32, side : side + 128] * inv[:, side : side + 128]
                mt[32 * h : 32 * h + 32, 128:256] = pltpu.roll(part, (128 - 16 * (h % 8)) % 128, 1)

    def half(par, win):
        new, old = par, 1 - par
        qrow = pl.multiple_of(jnp.clip(win, 0, 15) * TOK, 16)
        vrow = pl.multiple_of(jnp.clip(win - 2, 0, 15) * TOK, 16)
        xq = x2[new]
        xq[0:128] = x_ref[pl.ds(qrow, 128), :]
        few = x_ref[pl.ds(qrow + 128, 16), :]
        for t in range(8):
            xq[128 + 16 * t : 144 + 16 * t] = few
        krow = pl.multiple_of(jnp.clip(win - 1, 0, 15) * TOK, 16)
        soft = jnp.clip(win - 2, 0, 15)
        for n in range(9):
            if n < 2:
                project(q2[new], xq[...], 0, n)
            elif n < 4:
                project(v2[new], x_ref[pl.ds(vrow, TOK), :], 2 * D, n - 2)
            scores(q2[old], s2[old], krow, n)
            soften(s2[new], p2[new], soft, n)
            mix(v2[old], p2[old], m2[old], n)
        out_ref[old] = m2[old][...].T[0:TOK].astype(BF16)

    half(1, 2 * i - 1)
    half(0, 2 * i)


def far(array):
    return pltpu.with_memory_space_constraint(array, pltpu.HBM)


def attend(pos, x, bias, pieces):
    whole = lambda a: pl.BlockSpec(a.shape, lambda i: (0,) * a.ndim, pipeline_mode=pl.Buffered(1))
    return pl.pallas_call(
        attn_kernel,
        grid=(10,),
        in_specs=[
            pl.BlockSpec(memory_space=pltpu.SMEM),
            whole(x),
            whole(bias),
            *[whole(p) for p in pieces],
        ],
        out_specs=pl.BlockSpec((2, TOK, D), lambda i: (jnp.clip(i - 2, 0, 7), 0, 0)),
        out_shape=jax.ShapeDtypeStruct((16, TOK, D), BF16),
        scratch_shapes=[
            pltpu.VMEM((3 * D, D), BF16),
            pltpu.VMEM((16 * TOK, D), BF16),
            pltpu.VMEM((256, 128), BF16),
            *[pltpu.VMEM((D, 256), BF16)] * 4,
            *[pltpu.VMEM((TOK, 2304), F32)] * 2,
            *[pltpu.VMEM((TOK, 2304), BF16)] * 2,
            *[pltpu.VMEM((D, 256), F32)] * 2,
            *[pltpu.VMEM((256, D), BF16)] * 2,
        ],
        name="attend",
        compiler_params=pltpu.CompilerParams(vmem_limit_bytes=36 * 2**20),
        cost_estimate=pl.CostEstimate(flops=20_000_000_000, bytes_accessed=12_000_000, transcendentals=5_000_000),
    )(pos, far(x), far(bias), *pieces)


def mlp_kernel(pos_ref, mixed_ref, f_ref, gain_ref, *refs):
    pieces, out_ref, sent, (wp, wu, wd, held, normed) = refs[:4], refs[4], refs[5:-5], refs[-5:]

    @pl.when(pl.program_id(0) == 0)
    def _():
        for d3 in range(4):
            for d2 in range(4):
                for side in range(2):
                    b = rest_rows(pos_ref, side, d2, d3)
                    piece = pieces[d3].at[d2, side]
                    wp[pl.ds(pl.multiple_of(b * 16, 16), 16), :] = piece[0:16]
                    wu[pl.ds(pl.multiple_of(b * 64, 16), 64), :] = piece[16:80]
                    for c in range(4):
                        wd[c, pl.ds(pl.multiple_of(b * 16, 16), 16), :] = piece[80 + 16 * c : 96 + 16 * c]

    rows = out_ref.shape[0]
    sub = rows // 2

    def first(j):
        r = slice(j * sub, (j + 1) * sub)
        attn = lax.dot_general(mixed_ref[r], wp[...], NT, preferred_element_type=F32).astype(BF16)
        resid = (f_ref[r].astype(F32) + attn.astype(F32)).astype(BF16)
        held[r] = resid
        normed[r] = norm(resid.astype(F32), gain_ref[...])

    def second(j):
        r = slice(j * sub, (j + 1) * sub)
        total = None
        for c in range(4):
            pre = lax.dot_general(normed[r], wu[512 * c : 512 * c + 512, :], NT, preferred_element_type=F32)
            hidden = (0.5 * pre * (1.0 + lax.erf(pre * math.sqrt(0.5)))).astype(BF16)
            part = lax.dot_general(hidden, wd[c], NT, preferred_element_type=F32)
            total = part if total is None else total + part
        out_ref[r] = (held[r].astype(F32) + total).astype(BF16)

    first(0)
    first(1)
    second(0)
    second(1)
    if sent:
        lat_ref, lon_ref, diag_ref = sent
        corner = 3 * TOK
        for n in range(3):
            lat_ref[80 * n : 80 * n + 80] = out_ref[TOK * n + 64 : TOK * n + 144]
            lon_ref[80 * n : 80 * n + 80] = out_ref[TOK * n + 4 * TOK + 64 : TOK * n + 5 * TOK]
        lat_ref[240:320] = out_ref[corner + 32 : corner + 112]
        lon_ref[240:320] = out_ref[corner + 64 : corner + 144]
        diag_ref[...] = out_ref[corner + 96 : corner + 144]


def mlp(pos, mixed, f, gain, pieces, first, rows, sent=()):
    run = pl.BlockSpec((pl.Element(rows), pl.Element(D)), lambda i: (first, 0), pipeline_mode=pl.Buffered(1))
    whole = lambda a: pl.BlockSpec(a.shape, lambda i: (0,) * a.ndim, pipeline_mode=pl.Buffered(1))
    return pl.pallas_call(
        mlp_kernel,
        grid=(1,),
        in_specs=[
            pl.BlockSpec(memory_space=pltpu.SMEM),
            run,
            run,
            whole(gain),
            *[whole(p) for p in pieces],
        ],
        out_specs=[pl.BlockSpec((n, D), lambda i: (0, 0)) for n in (rows, *sent)],
        out_shape=[jax.ShapeDtypeStruct((n, D), BF16) for n in (rows, *sent)],
        scratch_shapes=[
            pltpu.VMEM((D, D), BF16),
            pltpu.VMEM((FF, D), BF16),
            pltpu.VMEM((4, D, D), BF16),
            pltpu.VMEM((rows, D), BF16),
            pltpu.VMEM((rows, D), BF16),
        ],
        compiler_params=pltpu.CompilerParams(vmem_limit_bytes=26 * 2**20),
        cost_estimate=pl.CostEstimate(
            flops=rows * 5_000_000, bytes_accessed=rows * 3072 + 5_000_000, transcendentals=rows * 2048
        ),
    )(pos, mixed, f, gain, *pieces)


def place_matrices():
    top = np.zeros((288, 368), np.float32)
    mid = np.zeros((576, 656), np.float32)
    for lev in range(2):
        for rr in range(3):
            for c in range(48):
                o = lev * 144 + rr * 48 + c
                at = lev * 18 + rr * 6
                wj, cc = (c - 6) // 12, (c - 6) % 12
                ch, c1 = cc // 6, cc % 6
                if c < 6:
                    top[o, 320 + 12 + at + c] = 1
                    for rh in range(2):
                        mid[rh * 288 + o, 576 + 8 + 36 * rh + at + c] = 1
                elif wj < 3:
                    top[o, 80 * wj + 8 + 36 * ch + at + c1] = 1
                    for rh in range(2):
                        mid[rh * 288 + o, 144 * wj + 72 * rh + 36 * ch + at + c1] = 1
                else:
                    top[o, 240 + 4 + at + c1] = 1
                    for rh in range(2):
                        mid[rh * 288 + o, 432 + 36 * rh + at + c1] = 1
    return top, mid


def place_kernel(edge_ref, inner_ref, lat_ref, lon_ref, diag_ref, top_ref, mid_ref, out_ref):
    def put(k, rows):
        for lev in range(2):
            for rr in range(3):
                at = lev * 144 + rr * 48
                out_ref[0, lev, 3 * k + rr] = rows[at : at + 48].astype(BF16)

    first = jnp.concatenate([lat_ref[...], diag_ref[...]], axis=0)
    put(0, jnp.dot(top_ref[...], first, preferred_element_type=F32))
    for wi in range(4):
        if wi < 3:
            three = inner_ref[432 * wi : 432 * wi + 432]
            last = edge_ref[576 + 144 * wi : 720 + 144 * wi]
        else:
            three = edge_ref[0:432]
            last = edge_ref[432:576]
        stack = jnp.concatenate([three, last, lon_ref[80 * wi : 80 * wi + 80]], axis=0)
        both = 576 if wi < 3 else 288
        rows = jnp.dot(mid_ref[0:both], stack, preferred_element_type=F32)
        put(1 + 2 * wi, rows[0:288])
        if wi < 3:
            put(2 + 2 * wi, rows[288:576])


def to_grid(edge, inner, lat, lon, diag):
    top, mid = place_matrices()
    return pl.pallas_call(
        place_kernel,
        out_shape=jax.ShapeDtypeStruct((1, 2, 24, 48, D), BF16),
        name="to_grid",
        compiler_params=pltpu.CompilerParams(vmem_limit_bytes=20 * 2**20),
        cost_estimate=pl.CostEstimate(flops=3_000_000_000, bytes_accessed=8_000_000, transcendentals=0),
    )(edge, inner, lat, lon, diag, jnp.asarray(top, BF16), jnp.asarray(mid, BF16))


def widen(own, stage):
    return jnp.stack([own, *[stage(own, d) for d in (1, 2, 3)]])


def body(fields, region, gain_attn, w_qkv, w_proj, gain_mlp, w_up, w_down):
    lat, lon = lax.axis_index("lat"), lax.axis_index("lon")
    mem = lax.axis_index("mem")
    pos = jnp.stack([(lon // 4) * 2 + mem // 2, lat, mem % 2]).astype(jnp.int32)

    down = w_down.T.reshape(4, 4, D).transpose(1, 0, 2).reshape(16, D)
    block = jnp.concatenate([w_qkv.T, w_proj.T, w_up.T, down], axis=0)
    line = widen(block, along_x)
    line = lax.dynamic_slice_in_dim(jnp.concatenate([line, line]), (4 - lon % 4) % 4, 4)
    stage = jnp.concatenate(
        [
            line[:, 0:12].reshape(48, D),
            line[:, 12:16].reshape(16, D),
            line[:, 16:32].reshape(64, D),
            line[:, 32:48].reshape(4, 4, 4, D).transpose(1, 0, 2, 3).reshape(64, D),
        ]
    )

    member = fields[0]
    _, clat, clon, _ = member.shape
    row = lax.broadcasted_iota(jnp.int32, (clat, clon), 0)
    ids = (region * 2 + ((lat == 0) & (row < SH)).astype(jnp.int32)).astype(BF16)

    def payload(part, marks, top, left):
        marks = jnp.pad(marks, ((top, 32 - top - marks.shape[0]), (left, D - left - marks.shape[1])))
        return jnp.concatenate([part.reshape(-1, D), marks])

    rows = from_grid(payload(member[:, :SH], ids[:SH], clat, 0), 1, 0)
    cols = from_grid(payload(member[:, :, :8], ids[:, :8], 0, clon), 0, 1)
    both = from_grid(payload(member[:, :SH, :8], ids[:SH, :8], clat, clon), 1, 1)
    ids = jnp.pad(ids, ((0, 32 - clat), (0, 128 - clon)))

    stage = jnp.concatenate([stage, other_core(stage[48:192])])
    firsts = [along_first(stage, d) for d in (1, 2, 3)]
    f, x, bias = prep(member, rows, cols, both, ids, gain_attn.reshape(1, D))
    firsts = lax.optimization_barrier((*firsts, f))[:3]
    group = jnp.stack([p[0:48] for p in (stage, *firsts)])
    rest = jnp.stack([p[48:336].reshape(2, 144, D) for p in (stage, *firsts)])
    qkv_sent = [along_second(group, d) for d in (1, 2, 3)]
    qkv_mine = jnp.stack([group, *qkv_sent])
    qkv_pieces = [qkv_mine, other_core(qkv_mine)]
    rest_mine = [rest, *[along_second(rest, d) for d in (1, 2, 3)]]
    mixed = attend(pos, x.reshape(-1, D), bias, qkv_pieces).reshape(-1, D)
    rest_pieces = lax.optimization_barrier((*rest_mine, mixed))[:4]
    f = f.reshape(-1, D)
    gain = gain_mlp.reshape(1, D)
    edge, lat_out, lon_out, diag_out = mlp(pos, mixed, f, gain, rest_pieces, 0, EDGE * TOK, (320, 320, 48))
    lat_in = from_grid(lat_out, -1, 0)
    lon_in = from_grid(lon_out, 0, -1)
    diag_in = from_grid(diag_out, -1, -1)
    (inner,) = mlp(pos, mixed, f, gain, rest_pieces, EDGE * TOK, INNER * TOK)
    return to_grid(edge, inner, lat_in, lon_in, diag_in)


def solution(mesh):
    weight = P(None, AXES)
    in_specs = (
        P("mem", None, "lat", "lon", None),
        P("lat", "lon"),
        P(),
        weight,
        weight,
        P(),
        weight,
        weight,
    )
    out_specs = P("mem", None, "lat", "lon", None)
    return jax.shard_map(body, mesh=mesh, in_specs=in_specs, out_specs=out_specs, check_vma=False)
```

```python
import math

import jax
import jax.numpy as jnp
import numpy as np
from jax import lax
from jax.experimental import pallas as pl
from jax.experimental.pallas import tpu as pltpu
from jax.sharding import PartitionSpec as P


D = 512
HDIM = 32
FF = 2048
SH = 3
SL = 6
TOK = 144
EDGE = 7
INNER = 9
AXES = ("mem", "lat", "lon")
MASKED = -1e30
EXP2_SCALE = math.log2(math.e) / math.sqrt(HDIM)
BF16 = jnp.bfloat16
F32 = jnp.float32
NT = (((1,), (1,)), ((), ()))

eps = 1e-05


def place(j):
    return j & 3, ((j >> 2) & 1) * 2 + ((j >> 6) & 1), (j >> 3) & 3, (j >> 5) & 1


def flat(x, y, z, core):
    return ((y & 1) << 6) | (core << 5) | (z << 3) | ((y >> 1) << 2) | x


def send(block, source_of):
    pairs = [(flat(*source_of(*place(j))), j) for j in range(128)]
    return lax.ppermute(block, AXES, pairs)


def along_x(block, d):
    return send(block, lambda x, y, z, c: ((x + d) % 4, y, z, c))


def along_first(block, d):
    return send(block, lambda x, y, z, c: (x, (y + d * (1 - c)) % 4, (z + d * c) % 4, c))


def along_second(block, d):
    return send(block, lambda x, y, z, c: (x, (y + d * c) % 4, (z + d * (1 - c)) % 4, c))


def other_core(block):
    return send(block, lambda x, y, z, c: (x, y, z, 1 - c))


def from_grid(block, dlat, dlon):
    pairs = []
    for j in range(128):
        mem, lat, lon = j >> 5, (j >> 3) & 3, j & 7
        pairs.append((mem * 32 + ((lat + dlat) % 4) * 8 + (lon + dlon) % 8, j))
    return lax.ppermute(block, AXES, pairs)


def norm(values, gain):
    average = jnp.mean(values, axis=-1, keepdims=True)
    centred = values - average
    variance = jnp.mean(centred * centred, axis=-1, keepdims=True)
    return (centred * lax.rsqrt(variance + eps) * gain).astype(BF16)


def prep_kernel(member_ref, rows_ref, cols_ref, both_ref, ids_ref, gain_ref, f_ref, x_ref, bias_ref, ext, near_ref):
    step = pl.program_id(0)

    @pl.when(step == 0)
    def _():
        ext[:, 0:24, 0:48] = member_ref[...]
        for lev in range(2):
            for n in range(24):
                at = (24 * lev + n) * 8
                ext[lev, n, 48:56] = cols_ref[at : at + 8]
            for n in range(3):
                at = 3 * lev + n
                ext[lev, 24 + n, 0:48] = rows_ref[48 * at : 48 * at + 48]
                ext[lev, 24 + n, 48:56] = both_ref[8 * at : 8 * at + 8]
        ext[:, :, 56:64] = jnp.zeros((2, 27, 8, D), BF16)
        ids = ids_ref[...].astype(F32)
        for ref, at in ((rows_ref, 288), (cols_ref, 384), (both_ref, 48)):
            ids = ids + ref[at : at + 32, 0:128].astype(F32)
        near_ref[...] = jnp.concatenate([ids, jnp.zeros((96, 128), F32)], axis=0).T

    col = lax.broadcasted_iota(jnp.int32, (1, 384), 1)
    seg = col // 32
    lev = (seg >= 6).astype(jnp.int32)
    r = seg - 6 * lev
    rh = (r >= 3).astype(jnp.int32)
    lane = lax.broadcasted_iota(jnp.int32, (32, 128), 1)
    every = jnp.ones((128, 128), BF16)
    for at in range(4):
        i = 4 * step + at
        k = i - EDGE
        wi = jnp.where(i < 4, 3, jnp.where(i < EDGE, i - 4, k // 3))
        wj = jnp.where(i < 4, i, jnp.where(i < EDGE, 3, k % 3))
        base = jnp.where(wj < 2, 0, jnp.where(wj == 2, 16, 32))
        cc = col - seg * 32 - (12 * wj + SL - base)
        ch = (cc >= 6).astype(jnp.int32)
        quad = jnp.where(wj == 3, ch * 2 + rh, rh * 2 + ch)
        row = quad * 36 + lev * 18 + (r - 3 * rh) * 6 + cc - 6 * ch
        row = jnp.where((cc >= 0) & (cc < 12), row, -1)
        pick = (lax.broadcasted_iota(jnp.int32, (TOK, 384), 0) == row).astype(F32).astype(BF16)
        start = pl.multiple_of(base, 16)
        tokens = jnp.concatenate(
            [ext[n // 6, 6 * wi + SH + n % 6, pl.ds(start, 32), :] for n in range(12)], axis=0
        )
        f = jnp.dot(pick, tokens, preferred_element_type=F32)
        f_ref[at] = f.astype(BF16)
        x = norm(f, gain_ref[...])
        x_ref[at] = x
        near = near_ref[pl.ds(start, 32), :]
        marks = [jnp.where(lane == 6 * wi + SH + n, near, 0.0).astype(BF16) for n in range(6)]
        marks = jnp.dot(pick, jnp.concatenate(marks * 2, axis=0), preferred_element_type=F32)
        idk = jnp.dot(marks.astype(BF16), every, preferred_element_type=F32)
        idq = jnp.concatenate([idk[0:128]] + [idk[128:144]] * 8, axis=0).T[0:1]
        bias_ref[at] = jnp.where(jnp.concatenate([idk, idk], axis=1) == idq, 0.0, MASKED).astype(BF16)


def prep(*operands):
    n = EDGE + INNER
    whole = lambda a: pl.BlockSpec(a.shape, lambda i: (0,) * a.ndim, pipeline_mode=pl.Buffered(1))
    out = lambda *s: (jax.ShapeDtypeStruct((n, *s), BF16), pl.BlockSpec((4, *s), lambda i: (i, 0, 0)))
    shapes, specs = zip(out(TOK, D), out(TOK, D), out(TOK, 256))
    return pl.pallas_call(
        prep_kernel,
        grid=(n // 4,),
        in_specs=[whole(a) for a in operands],
        out_specs=specs,
        out_shape=shapes,
        scratch_shapes=[pltpu.VMEM((2, 27, 64, D), BF16), pltpu.VMEM((128, 128), F32)],
        name="prep",
        cost_estimate=pl.CostEstimate(flops=6_000_000_000, bytes_accessed=16_000_000, transcendentals=0),
    )(*operands)


def block_rows(pos_ref, side, d2, d3):
    core = pos_ref[2]
    core = core if side == 0 else 1 - core
    dy = jnp.where(core == 0, d2, d3)
    dz = jnp.where(core == 0, d3, d2)
    y = (pos_ref[0] + dy) % 4
    z = (pos_ref[1] + dz) % 4
    return (y % 2) * 16 + core * 8 + z * 2 + y // 2


def rest_rows(pos_ref, side, d2, d3):
    mine = pos_ref[2]
    dy = jnp.where(mine == 0, d2, d3)
    dz = jnp.where(mine == 0, d3, d2)
    y = (pos_ref[0] + dy) % 4
    z = (pos_ref[1] + dz) % 4
    return (y % 2) * 16 + (mine if side == 0 else 1 - mine) * 8 + z * 2 + y // 2


def attn_kernel(pos_ref, x_ref, bias_ref, *refs):
    pieces, out_ref = refs[:2], refs[2]
    w, kall, own = refs[3:6]
    q2, v2, s2, p2, m2, x2 = (refs[n : n + 2] for n in range(6, 18, 2))
    i = pl.program_id(0)

    @pl.when(i == 0)
    def _():
        for p in range(8):
            for d2 in range(4):
                b = block_rows(pos_ref, p // 4, d2, p % 4)
                w[pl.ds(pl.multiple_of(b * 48, 16), 48), :] = pieces[p // 4][p % 4, d2]
        keys = lax.dot_general(x_ref[...], w[D : 2 * D, :], NT, preferred_element_type=F32)
        kall[...] = keys.astype(BF16)
        own[...] = (
            lax.broadcasted_iota(jnp.int32, (256, 128), 0) // 32
            == lax.broadcasted_iota(jnp.int32, (256, 128), 1) // 16
        ).astype(F32).astype(BF16)

    ones = jnp.ones((16, TOK), BF16)
    zeros = jnp.zeros((32, 128), BF16)

    def project(dst, x, first, n):
        at = 256 * n
        out = lax.dot_general(w[first + at : first + at + 256, :], x, NT, preferred_element_type=F32)
        dst[at : at + 256, 0 : x.shape[0]] = out.astype(BF16)

    def scores(qt, s, krow, n):
        if n < 8:
            g = n // 2
            heads = []
            for h in (2 * (n % 2), 2 * (n % 2) + 1):
                q = qt[128 * g + 32 * h : 128 * g + 32 * h + 32, 0:128]
                heads.append(jnp.concatenate([zeros] * h + [q] + [zeros] * (3 - h), axis=0))
            kg = kall[pl.ds(krow, TOK), 128 * g : 128 * g + 128]
            s[:, 256 * n : 256 * n + 256] = jnp.dot(
                kg, jnp.concatenate(heads, axis=1), preferred_element_type=F32
            )
        else:
            for a in range(2):
                q = qt[256 * a : 256 * a + 256, 128:256] * own[...]
                s[:, 2048 + 128 * a : 2176 + 128 * a] = jnp.dot(
                    kall[pl.ds(krow, TOK), 256 * a : 256 * a + 256], q, preferred_element_type=F32
                )

    def soften(s, p, win, n):
        side = 0 if n < 8 else 128
        bias = bias_ref[win, :, side : side + 128].astype(F32)
        for at in (256 * n, 256 * n + 128):
            v = s[:, at : at + 128] + bias
            m = jnp.max(v, axis=0, keepdims=True)
            p[:, at : at + 128] = jnp.exp2((v - m) * EXP2_SCALE).astype(BF16)

    def mix(vt, p, mt, n):
        at = 64 * n
        if n < 8:
            lhs = jnp.concatenate([vt[at : at + 64, 0:TOK], ones], axis=0)
            o = jnp.dot(lhs, p[:, 256 * n : 256 * n + 256], preferred_element_type=F32)
            inv = 1.0 / o[64:65]
            mt[at : at + 32, 0:128] = o[0:32, 0:128] * inv[:, 0:128]
            mt[at + 32 : at + 64, 0:128] = o[32:64, 128:256] * inv[:, 128:256]
        else:
            lhs = jnp.concatenate([vt[:, 0:TOK], ones], axis=0)
            o = jnp.dot(lhs, p[:, 2048:2304], preferred_element_type=F32)
            inv = 1.0 / o[D : D + 1]
            for h in range(16):
                side = 128 * (h // 8)
                part = o[32 * h : 32 * h + 32, side : side + 128] * inv[:, side : side + 128]
                mt[32 * h : 32 * h + 32, 128:256] = pltpu.roll(part, (128 - 16 * (h % 8)) % 128, 1)

    def half(par, win):
        new, old = par, 1 - par
        qrow = pl.multiple_of(jnp.clip(win, 0, 15) * TOK, 16)
        vrow = pl.multiple_of(jnp.clip(win - 2, 0, 15) * TOK, 16)
        xq = x2[new]
        xq[0:128] = x_ref[pl.ds(qrow, 128), :]
        few = x_ref[pl.ds(qrow + 128, 16), :]
        for t in range(8):
            xq[128 + 16 * t : 144 + 16 * t] = few
        krow = pl.multiple_of(jnp.clip(win - 1, 0, 15) * TOK, 16)
        soft = jnp.clip(win - 2, 0, 15)
        for n in range(9):
            if n < 2:
                project(q2[new], xq[...], 0, n)
            elif n < 4:
                project(v2[new], x_ref[pl.ds(vrow, TOK), :], 2 * D, n - 2)
            scores(q2[old], s2[old], krow, n)
            soften(s2[new], p2[new], soft, n)
            mix(v2[old], p2[old], m2[old], n)
        out_ref[old] = m2[old][...].T[0:TOK].astype(BF16)

    half(1, 2 * i - 1)
    half(0, 2 * i)


def far(array):
    return pltpu.with_memory_space_constraint(array, pltpu.HBM)


def attend(pos, x, bias, pieces):
    whole = lambda a: pl.BlockSpec(a.shape, lambda i: (0,) * a.ndim, pipeline_mode=pl.Buffered(1))
    return pl.pallas_call(
        attn_kernel,
        grid=(10,),
        in_specs=[
            pl.BlockSpec(memory_space=pltpu.SMEM),
            whole(x),
            whole(bias),
            *[whole(p) for p in pieces],
        ],
        out_specs=pl.BlockSpec((2, TOK, D), lambda i: (jnp.clip(i - 2, 0, 7), 0, 0)),
        out_shape=jax.ShapeDtypeStruct((16, TOK, D), BF16),
        scratch_shapes=[
            pltpu.VMEM((3 * D, D), BF16),
            pltpu.VMEM((16 * TOK, D), BF16),
            pltpu.VMEM((256, 128), BF16),
            *[pltpu.VMEM((D, 256), BF16)] * 4,
            *[pltpu.VMEM((TOK, 2304), F32)] * 2,
            *[pltpu.VMEM((TOK, 2304), BF16)] * 2,
            *[pltpu.VMEM((D, 256), F32)] * 2,
            *[pltpu.VMEM((256, D), BF16)] * 2,
        ],
        name="attend",
        compiler_params=pltpu.CompilerParams(vmem_limit_bytes=36 * 2**20),
        cost_estimate=pl.CostEstimate(flops=20_000_000_000, bytes_accessed=12_000_000, transcendentals=5_000_000),
    )(pos, far(x), far(bias), *pieces)


def mlp_kernel(pos_ref, mixed_ref, f_ref, gain_ref, *refs):
    pieces, out_ref, sent, (wp, wu, wd, held, normed) = refs[:4], refs[4], refs[5:-5], refs[-5:]

    @pl.when(pl.program_id(0) == 0)
    def _():
        for d3 in range(4):
            for d2 in range(4):
                for side in range(2):
                    b = rest_rows(pos_ref, side, d2, d3)
                    piece = pieces[d3].at[d2, side]
                    wp[pl.ds(pl.multiple_of(b * 16, 16), 16), :] = piece[0:16]
                    wu[pl.ds(pl.multiple_of(b * 64, 16), 64), :] = piece[16:80]
                    for c in range(4):
                        wd[c, pl.ds(pl.multiple_of(b * 16, 16), 16), :] = piece[80 + 16 * c : 96 + 16 * c]

    rows = out_ref.shape[0]
    sub = rows // 2

    def first(j):
        r = slice(j * sub, (j + 1) * sub)
        attn = lax.dot_general(mixed_ref[r], wp[...], NT, preferred_element_type=F32).astype(BF16)
        resid = (f_ref[r].astype(F32) + attn.astype(F32)).astype(BF16)
        held[r] = resid
        normed[r] = norm(resid.astype(F32), gain_ref[...])

    def second(j):
        r = slice(j * sub, (j + 1) * sub)
        total = None
        for c in range(2):
            pre = lax.dot_general(normed[r], wu[1024 * c : 1024 * c + 1024, :], NT, preferred_element_type=F32)
            hidden = (0.5 * pre * (1.0 + lax.erf(pre * math.sqrt(0.5)))).astype(BF16)
            for k in range(2):
                part = lax.dot_general(
                    hidden[:, 512 * k : 512 * k + 512], wd[2 * c + k], NT, preferred_element_type=F32
                )
                total = part if total is None else total + part
        out_ref[r] = (held[r].astype(F32) + total).astype(BF16)

    first(0)
    first(1)
    second(0)
    second(1)
    if sent:
        lat_ref, lon_ref, diag_ref = sent
        corner = 3 * TOK
        for n in range(3):
            lat_ref[80 * n : 80 * n + 80] = out_ref[TOK * n + 64 : TOK * n + 144]
            lon_ref[80 * n : 80 * n + 80] = out_ref[TOK * n + 4 * TOK + 64 : TOK * n + 5 * TOK]
        lat_ref[240:320] = out_ref[corner + 32 : corner + 112]
        lon_ref[240:320] = out_ref[corner + 64 : corner + 144]
        diag_ref[...] = out_ref[corner + 96 : corner + 144]


def mlp(pos, mixed, f, gain, pieces, first, rows, sent=()):
    run = pl.BlockSpec((pl.Element(rows), pl.Element(D)), lambda i: (first, 0), pipeline_mode=pl.Buffered(1))
    whole = lambda a: pl.BlockSpec(a.shape, lambda i: (0,) * a.ndim, pipeline_mode=pl.Buffered(1))
    return pl.pallas_call(
        mlp_kernel,
        grid=(1,),
        in_specs=[
            pl.BlockSpec(memory_space=pltpu.SMEM),
            run,
            run,
            whole(gain),
            *[whole(p) for p in pieces],
        ],
        out_specs=[pl.BlockSpec((n, D), lambda i: (0, 0)) for n in (rows, *sent)],
        out_shape=[jax.ShapeDtypeStruct((n, D), BF16) for n in (rows, *sent)],
        scratch_shapes=[
            pltpu.VMEM((D, D), BF16),
            pltpu.VMEM((FF, D), BF16),
            pltpu.VMEM((4, D, D), BF16),
            pltpu.VMEM((rows, D), BF16),
            pltpu.VMEM((rows, D), BF16),
        ],
        compiler_params=pltpu.CompilerParams(vmem_limit_bytes=26 * 2**20),
        cost_estimate=pl.CostEstimate(
            flops=rows * 5_000_000, bytes_accessed=rows * 3072 + 5_000_000, transcendentals=rows * 2048
        ),
    )(pos, mixed, f, gain, *pieces)


def place_matrices():
    top = np.zeros((288, 368), np.float32)
    mid = np.zeros((576, 656), np.float32)
    for lev in range(2):
        for rr in range(3):
            for c in range(48):
                o = lev * 144 + rr * 48 + c
                at = lev * 18 + rr * 6
                wj, cc = (c - 6) // 12, (c - 6) % 12
                ch, c1 = cc // 6, cc % 6
                if c < 6:
                    top[o, 320 + 12 + at + c] = 1
                    for rh in range(2):
                        mid[rh * 288 + o, 576 + 8 + 36 * rh + at + c] = 1
                elif wj < 3:
                    top[o, 80 * wj + 8 + 36 * ch + at + c1] = 1
                    for rh in range(2):
                        mid[rh * 288 + o, 144 * wj + 72 * rh + 36 * ch + at + c1] = 1
                else:
                    top[o, 240 + 4 + at + c1] = 1
                    for rh in range(2):
                        mid[rh * 288 + o, 432 + 36 * rh + at + c1] = 1
    return top, mid


def place_kernel(edge_ref, inner_ref, lat_ref, lon_ref, diag_ref, top_ref, mid_ref, out_ref):
    def put(k, rows):
        for lev in range(2):
            for rr in range(3):
                at = lev * 144 + rr * 48
                out_ref[0, lev, 3 * k + rr] = rows[at : at + 48].astype(BF16)

    first = jnp.concatenate([lat_ref[...], diag_ref[...]], axis=0)
    put(0, jnp.dot(top_ref[...], first, preferred_element_type=F32))
    for wi in range(4):
        if wi < 3:
            three = inner_ref[432 * wi : 432 * wi + 432]
            last = edge_ref[576 + 144 * wi : 720 + 144 * wi]
        else:
            three = edge_ref[0:432]
            last = edge_ref[432:576]
        stack = jnp.concatenate([three, last, lon_ref[80 * wi : 80 * wi + 80]], axis=0)
        both = 576 if wi < 3 else 288
        rows = jnp.dot(mid_ref[0:both], stack, preferred_element_type=F32)
        put(1 + 2 * wi, rows[0:288])
        if wi < 3:
            put(2 + 2 * wi, rows[288:576])


def to_grid(edge, inner, lat, lon, diag):
    top, mid = place_matrices()
    return pl.pallas_call(
        place_kernel,
        out_shape=jax.ShapeDtypeStruct((1, 2, 24, 48, D), BF16),
        name="to_grid",
        compiler_params=pltpu.CompilerParams(vmem_limit_bytes=20 * 2**20),
        cost_estimate=pl.CostEstimate(flops=3_000_000_000, bytes_accessed=8_000_000, transcendentals=0),
    )(edge, inner, lat, lon, diag, jnp.asarray(top, BF16), jnp.asarray(mid, BF16))


def widen(own, stage):
    return jnp.stack([own, *[stage(own, d) for d in (1, 2, 3)]])


def body(fields, region, gain_attn, w_qkv, w_proj, gain_mlp, w_up, w_down):
    lat, lon = lax.axis_index("lat"), lax.axis_index("lon")
    mem = lax.axis_index("mem")
    pos = jnp.stack([(lon // 4) * 2 + mem // 2, lat, mem % 2]).astype(jnp.int32)

    down = w_down.T.reshape(4, 4, D).transpose(1, 0, 2).reshape(16, D)
    block = jnp.concatenate([w_qkv.T, w_proj.T, w_up.T, down], axis=0)
    line = widen(block, along_x)
    line = lax.dynamic_slice_in_dim(jnp.concatenate([line, line]), (4 - lon % 4) % 4, 4)
    stage = jnp.concatenate(
        [
            line[:, 0:12].reshape(48, D),
            line[:, 12:16].reshape(16, D),
            line[:, 16:32].reshape(64, D),
            line[:, 32:48].reshape(4, 4, 4, D).transpose(1, 0, 2, 3).reshape(64, D),
        ]
    )

    member = fields[0]
    _, clat, clon, _ = member.shape
    row = lax.broadcasted_iota(jnp.int32, (clat, clon), 0)
    ids = (region * 2 + ((lat == 0) & (row < SH)).astype(jnp.int32)).astype(BF16)

    def payload(part, marks, top, left):
        marks = jnp.pad(marks, ((top, 32 - top - marks.shape[0]), (left, D - left - marks.shape[1])))
        return jnp.concatenate([part.reshape(-1, D), marks])

    rows = from_grid(payload(member[:, :SH], ids[:SH], clat, 0), 1, 0)
    cols = from_grid(payload(member[:, :, :8], ids[:, :8], 0, clon), 0, 1)
    both = from_grid(payload(member[:, :SH, :8], ids[:SH, :8], clat, clon), 1, 1)
    ids = jnp.pad(ids, ((0, 32 - clat), (0, 128 - clon)))

    stage = jnp.concatenate([stage, other_core(stage[48:192])])
    firsts = [along_first(stage, d) for d in (1, 2, 3)]
    f, x, bias = prep(member, rows, cols, both, ids, gain_attn.reshape(1, D))
    firsts = lax.optimization_barrier((*firsts, f))[:3]
    group = jnp.stack([p[0:48] for p in (stage, *firsts)])
    rest = jnp.stack([p[48:336].reshape(2, 144, D) for p in (stage, *firsts)])
    qkv_sent = [along_second(group, d) for d in (1, 2, 3)]
    qkv_mine = jnp.stack([group, *qkv_sent])
    qkv_pieces = [qkv_mine, other_core(qkv_mine)]
    rest_mine = [rest, *[along_second(rest, d) for d in (1, 2, 3)]]
    mixed = attend(pos, x.reshape(-1, D), bias, qkv_pieces).reshape(-1, D)
    rest_pieces = lax.optimization_barrier((*rest_mine, mixed))[:4]
    f = f.reshape(-1, D)
    gain = gain_mlp.reshape(1, D)
    edge, lat_out, lon_out, diag_out = mlp(pos, mixed, f, gain, rest_pieces, 0, EDGE * TOK, (320, 320, 48))
    lat_in = from_grid(lat_out, -1, 0)
    lon_in = from_grid(lon_out, 0, -1)
    diag_in = from_grid(diag_out, -1, -1)
    (inner,) = mlp(pos, mixed, f, gain, rest_pieces, EDGE * TOK, INNER * TOK)
    return to_grid(edge, inner, lat_in, lon_in, diag_in)


def solution(mesh):
    weight = P(None, AXES)
    in_specs = (
        P("mem", None, "lat", "lon", None),
        P("lat", "lon"),
        P(),
        weight,
        weight,
        P(),
        weight,
        weight,
    )
    out_specs = P("mem", None, "lat", "lon", None)
    return jax.shard_map(body, mesh=mesh, in_specs=in_specs, out_specs=out_specs, check_vma=False)
```
